32 devices in a mesh: groups: 2 (over x), az: 16 (over z, y, core).
Axes of the slice: x: 2, y: 2, z: 4, core: 2. Of those that a mesh axis runs over, the one named last changes fastest.
Arguments:
- raw_first: bfloat16 [4, 8192, 8192], P('groups', 'az'), parts along dimension 0, may hold values from -6 to 6
- raw_second: bfloat16 [4, 8192, 8192], P('groups', 'az'), parts along dimension 0, may hold values from -6 to 6
- offsets: int32 [4], P('groups'), parts along dimension 0, may hold values from -16 to 16
- chirp_lengths: int32 [4], P('groups'), parts along dimension 0, may hold values from 256 to 2048
Outputs:
- interferogram: float32 [4, 1024, 8192], P('groups', 'az'), parts along dimension 0
- coherence: float32 [2048, 8192], P(('groups', 'az')), parts along dimension 0
The draws below stay inside these ranges and needn't reach their ends.
There are 2 independent parts, one for each index of `groups`. The reference program is written for one: setup_inputs(seed, part) draws one part's arguments, and reference() takes and returns one part's arrays. A program takes and returns all parts, laid end to end along the dimension named above; each array names one. Nothing has to cross between parts.
Inputs may be any that keep to these rules, and one draw needn't show every extreme that they name: offsets[0] shifts azimuth lines, offsets[1] range bins. chirp_lengths[0] is the range chirp, chirp_lengths[1] the azimuth chirp.
All inputs are finite; a program needn't handle non-finite values.
Results may differ from the reference program's by a relative error of at most 0.0003.
Values sent between devices are 32-bit elements; how exact they have to be, the bound alone decides.
A program may use at most 256 MiB of HBM per device.

```python
import jax
import jax.numpy as jnp
from jax import lax

NAZ = 8192
NRG = 8192
WINDOW = 1024
MAXSHIFT = 16


def block_levels(key, shape, cuts, least, top_value):
    gain, own = 1.0, jax.random.fold_in(key, 6)
    for position, parts in cuts:
        heights = jnp.exp(jax.random.uniform(jax.random.fold_in(own, position), (parts,), jnp.float32, least / len(cuts), top_value / len(cuts)))
        gain = gain * jnp.repeat(heights, shape[position] // parts).reshape([-1 if axis == position else 1 for axis in range(len(shape))])
    return gain


def bell_draw(rng, dims, spread, limit, cuts=(), kind=jnp.bfloat16):
    loudness = block_levels(rng, dims, cuts, -0.22, 0.18) if cuts else 1.0
    drawn = jax.random.normal(rng, dims, jnp.float32) * spread * loudness
    return jnp.minimum(jnp.maximum(drawn, -limit), limit).astype(kind)


def setup_inputs(seed: int = 0, part: int = 0) -> dict:
    arg_keys = jax.random.split(jax.random.key(seed), 5)
    part_keys = jax.random.split(jax.random.fold_in(arg_keys[4], part), 5)
    raw_first = bell_draw(part_keys[0], (2, NAZ, NRG), 1.0, 6.0, ((1, 16),))
    raw_second = bell_draw(part_keys[1], (2, NAZ, NRG), 1.0, 6.0, ((1, 16),))
    offsets = jax.random.randint(part_keys[2], (2,), 0 - MAXSHIFT, MAXSHIFT + 1).astype(jnp.int32)
    chirp_lengths = jax.random.randint(part_keys[3], (2,), min(NRG, NAZ) // 32, min(NRG, NAZ) // 4 + 1).astype(jnp.int32)
    return dict(raw_first=raw_first, raw_second=raw_second, offsets=offsets, chirp_lengths=chirp_lengths)


def chirp(length, samples_all):
    sample = jnp.arange(samples_all, dtype=jnp.int32)
    offset = 2 * sample - length
    period = 8 * length
    numerator = jnp.mod(offset * offset, period)
    angles = jnp.pi * numerator.astype(jnp.float32) / (4 * length).astype(jnp.float32)
    amplitude = jnp.where(sample < length, 1.0 / jnp.sqrt(length.astype(jnp.float32)), 0.0).astype(jnp.float32)
    return (amplitude * jnp.cos(angles), amplitude * jnp.sin(angles))

def boxed(values):
    rows_count, cols_count = values.shape
    padded = jnp.pad(values, ((3, 4), (3, 4)))
    across = padded[0:rows_count]
    for offset_row in range(1, 8):
        across = across + padded[offset_row:offset_row + rows_count]
    result = across[:, 0:cols_count]
    for offset_col in range(1, 8):
        result = result + across[:, offset_col:offset_col + cols_count]
    return result

def focus(raw, range_filter, azimuth_filter):
    signal = lax.complex(raw[0].astype(jnp.float32), raw[1].astype(jnp.float32))
    signal = jnp.fft.ifft(jnp.fft.fft(signal, axis=1) * range_filter[None, :], axis=1)
    return jnp.fft.ifft(jnp.fft.fft(signal, axis=0) * azimuth_filter[:, None], axis=0)

def reference(raw_first, raw_second, offsets, chirp_lengths):
    range_real, range_imag = chirp(chirp_lengths[0], NRG)
    range_filter = jnp.conj(jnp.fft.fft(lax.complex(range_real, range_imag)))
    azimuth_real, azimuth_imag = chirp(chirp_lengths[1], NAZ)
    azimuth_filter = jnp.conj(jnp.fft.fft(lax.complex(azimuth_real, azimuth_imag)))
    first = focus(raw_first, range_filter, azimuth_filter)[:, 0:WINDOW]
    second = focus(raw_second, range_filter, azimuth_filter)
    padded = jnp.pad(second, MAXSHIFT)
    second = lax.dynamic_slice(padded, ((MAXSHIFT - offsets[0]).astype(jnp.int32), (MAXSHIFT - offsets[1]).astype(jnp.int32)), (NAZ, WINDOW))
    cross = first * jnp.conj(second)
    sums_real = boxed(jnp.real(cross))
    sums_imag = boxed(jnp.imag(cross))
    power_first = boxed(jnp.real(first) * jnp.real(first) + jnp.imag(first) * jnp.imag(first))
    power_second = boxed(jnp.real(second) * jnp.real(second) + jnp.imag(second) * jnp.imag(second))
    coherence = jnp.sqrt(sums_real * sums_real + sums_imag * sums_imag) / jnp.sqrt(power_first * power_second + 1.0)
    interferogram = jnp.stack([sums_real.T, sums_imag.T]) / 64.0
    return (interferogram, coherence.T)
```

```python
import functools
import math

import jax
import jax.numpy as jnp
import numpy as np
from jax import lax
from jax.experimental import pallas as pl
from jax.experimental.pallas import tpu as pltpu
from jax.sharding import PartitionSpec as P

WINDOW = 1024
MAXSHIFT = 16
LANES = 128
TILE = 256
VMEM_BYTES = 60 * 1024 * 1024


along_forms = (
    ("rij", "ik", "rkj"),
    ("rkj", "jl", "rkl"),
    ("rkl", "jl", "rkj"),
    ("rkj", "ik", "rij"),
)


def padded_2(block, sides, width):
    for axis, dim in sides:
        count = lax.axis_size(axis)
        forward = [(i, i + 1) for i in range(count - 1)]
        backward = [(target, source) for source, target in forward]
        low = lax.ppermute(
            lax.slice_in_dim(block, block.shape[dim] - width, None, axis=dim), axis, forward
        )
        high = lax.ppermute(lax.slice_in_dim(block, 0, width, axis=dim), axis, backward)
        block = jnp.concatenate([low, block, high], axis=dim)
    return block


def chirp(length, samples_all):
    sample = jnp.arange(samples_all, dtype=jnp.int32)
    offset = 2 * sample - length
    period = 8 * length
    numerator = jnp.mod(offset * offset, period)
    angles = jnp.pi * numerator.astype(jnp.float32) / (4 * length).astype(jnp.float32)
    amplitude = jnp.where(sample < length, 1.0 / jnp.sqrt(length.astype(jnp.float32)), 0.0)
    return (amplitude * jnp.cos(angles), amplitude * jnp.sin(angles))


def roots(rows_count, cols_count, period):
    product = lax.broadcasted_iota(jnp.int32, (rows_count, cols_count), 0) * lax.broadcasted_iota(
        jnp.int32, (rows_count, cols_count), 1
    )
    angles = -2.0 * math.pi / period * jnp.mod(product, period).astype(jnp.float32)
    return (jnp.cos(angles), jnp.sin(angles))


def tables(length):
    right_size = LANES
    left_size = length // right_size
    entries = (
        roots(left_size, left_size, left_size)
        + roots(right_size, right_size, right_size)
        + roots(left_size, right_size, length)
    )
    return (entries, left_size, right_size)


def complex_product(form, stacked, table_real, table_imag):
    left_side, right_side, result_side = form
    matrix = jnp.stack([jnp.stack([table_real, table_imag]), jnp.stack([-table_imag, table_real])])
    return jnp.einsum(
        "c" + left_side + ",cd" + right_side + "->d" + result_side,
        stacked,
        matrix,
        precision=lax.Precision.HIGHEST,
    )


def complex_times(stacked, other_real, other_imag):
    return jnp.stack(
        [
            stacked[0] * other_real - stacked[1] * other_imag,
            stacked[0] * other_imag + stacked[1] * other_real,
        ]
    )


def forward(stacked, entries, forms):
    left_real, left_imag, right_real, right_imag, twist_real, twist_imag = entries
    stacked = complex_product(forms[0], stacked, left_real, left_imag)
    stacked = complex_times(stacked, twist_real, twist_imag)
    return complex_product(forms[1], stacked, right_real, right_imag)


def split(values):
    high = values.astype(jnp.bfloat16)
    return high, (values - high.astype(jnp.float32)).astype(jnp.bfloat16)


def dot(left, right):
    return jnp.dot(left, right, preferred_element_type=jnp.float32)


def dot_split(left, right):
    return dot(left[0], right[0]) + (dot(left[0], right[1]) + dot(left[1], right[0]))


def chirp_segments(length, taps):
    place = lax.broadcasted_iota(jnp.int32, (taps, 2 * TILE), 1)
    sample = lax.broadcasted_iota(jnp.int32, (taps, 2 * TILE), 0) * TILE - place
    sample = jnp.where(place < TILE, sample, sample + 2 * TILE)
    offset = 2 * sample - length
    numerator = jnp.mod(offset * offset, 8 * length)
    angles = jnp.pi * numerator.astype(jnp.float32) / (4 * length).astype(jnp.float32)
    inside = (sample >= 0) & (sample < length)
    amplitude = jnp.where(inside, 1.0 / jnp.sqrt(length.astype(jnp.float32)), 0.0)
    return jnp.stack([amplitude * jnp.cos(angles), -amplitude * jnp.sin(angles)], axis=1)


def range_kernel(
    taps, shifted, shift_ref, seg_ref, raw_ref, out_ref, real_high, real_low, imag_high, imag_low,
    *rest,
):
    depth = taps * TILE

    @pl.when(pl.program_id(0) == 0)
    def _():
        for tap in range(taps):
            rows = pl.ds(tap * TILE, TILE)
            turned = []
            for part in range(2):
                row = jnp.broadcast_to(seg_ref[tap, pl.ds(part, 1), :], (TILE, 2 * TILE))
                turned.append(pltpu.roll(row, 0, 1, stride=1, stride_axis=0)[:, 0:TILE])
            for part, (columns, high_ref, low_ref) in enumerate(
                (
                    (0, real_high, real_low),
                    (TILE, real_high, real_low),
                )
            ):
                high, low = split(turned[part])
                high_ref[rows, pl.ds(columns, TILE)] = high
                low_ref[rows, pl.ds(columns, TILE)] = low
                if part == 0:
                    imag_high[rows, pl.ds(TILE, TILE)] = high
                    imag_low[rows, pl.ds(TILE, TILE)] = low
                else:
                    imag_high[rows, pl.ds(0, TILE)] = -high
                    imag_low[rows, pl.ds(0, TILE)] = -low
            if shifted:
                edge_real_high, edge_real_low, edge_imag_high, edge_imag_low = rest[1:]
                real, imag = turned[0][:, 0:LANES], turned[1][:, 0:LANES]
                low_half = lax.broadcasted_iota(jnp.int32, (TILE, LANES), 1) < LANES // 2
                high, low = split(jnp.where(low_half, real, pltpu.roll(imag, LANES // 2, 1)))
                edge_real_high[rows], edge_real_low[rows] = high, low
                high, low = split(jnp.where(low_half, -imag, pltpu.roll(real, LANES // 2, 1)))
                edge_imag_high[rows], edge_imag_low[rows] = high, low

    def correlated(start, tabs):
        columns = pl.ds(start, depth)
        real, imag = raw_ref[0, :, columns], raw_ref[1, :, columns]
        return (dot(real, tabs[0][...]) + dot(imag, tabs[2][...])) + (
            dot(real, tabs[1][...]) + dot(imag, tabs[3][...])
        )

    tabs = (real_high, real_low, imag_high, imag_low)
    bins = out_ref.shape[2]
    for block in range(WINDOW // TILE):
        result = correlated(block * TILE, tabs)
        for part in range(2):
            turned = result[:, part * TILE : (part + 1) * TILE].T
            if shifted:
                rest[0][part, pl.ds(MAXSHIFT + block * TILE, TILE), :] = turned
            else:
                out_ref[pl.ds(block * TILE // bins, TILE // bins), part] = turned.reshape(
                    TILE // bins, bins, turned.shape[1]
                )
    if shifted:
        target = rest[0]
        edge = correlated(WINDOW, rest[1:]).T
        for part in range(2):
            target[part, 0:MAXSHIFT, :] = jnp.zeros((MAXSHIFT, edge.shape[1]), jnp.float32)
            target[part, pl.ds(MAXSHIFT + WINDOW, MAXSHIFT), :] = edge[
                part * LANES // 2 : part * LANES // 2 + MAXSHIFT
            ]
        held = WINDOW + 2 * MAXSHIFT
        turn = lax.rem(held - MAXSHIFT + shift_ref[0], held)
        for part in range(2):
            moved = pltpu.roll(target[part], turn, 0)[0:WINDOW]
            out_ref[:, part] = moved.reshape(WINDOW // bins, bins, moved.shape[1])


def range_focus(raw, segments, shift, shifted):
    parts = lax.axis_size("az")
    bins = WINDOW // parts
    taps = segments.shape[0]
    depth = taps * TILE
    lines_count = raw.shape[1]
    height = min(TILE, lines_count)
    width = depth + WINDOW
    scratch = [pltpu.VMEM((depth, 2 * TILE), jnp.bfloat16)] * 4
    if shifted:
        scratch += [pltpu.VMEM((2, WINDOW + 2 * MAXSHIFT, height), jnp.float32)]
        scratch += [pltpu.VMEM((depth, LANES), jnp.bfloat16)] * 4
    return pl.pallas_call(
        functools.partial(range_kernel, taps, shifted),
        out_shape=jax.ShapeDtypeStruct((parts, 2, bins, lines_count), jnp.float32),
        grid=(lines_count // height,),
        in_specs=[
            pl.BlockSpec(memory_space=pltpu.SMEM),
            pl.BlockSpec((taps, 2, 2 * TILE), lambda i: (0, 0, 0)),
            pl.BlockSpec((2, height, width), lambda i: (0, i, 0)),
        ],
        out_specs=pl.BlockSpec((parts, 2, bins, height), lambda i: (0, 0, 0, i)),
        scratch_shapes=scratch,
        compiler_params=pltpu.CompilerParams(vmem_limit_bytes=VMEM_BYTES),
        cost_estimate=pl.CostEstimate(
            flops=16 * lines_count * depth * WINDOW,
            bytes_accessed=4 * lines_count * (width + 2 * WINDOW),
            transcendentals=0,
        ),
        name="range_second" if shifted else "range_first",
    )(shift, segments, raw)


def azimuth_image(in_ref, spec_ref, left_ref, right_ref, twist_ref):
    parts, _, bins, lines_count = in_ref.shape
    lines = parts * lines_count
    left_size = lines // LANES
    real, imag = (
        jnp.concatenate([in_ref[one, part] for one in range(parts)], axis=1).reshape(
            bins, left_size, LANES
        )
        for part in range(2)
    )
    twist_real, twist_imag = twist_ref[0], twist_ref[1]
    middle_real, middle_imag = [], []
    for one in range(0, bins, 2):
        pair = jnp.concatenate(
            [
                jnp.concatenate([real[one], imag[one]], axis=0),
                jnp.concatenate([real[one + 1], imag[one + 1]], axis=0),
            ],
            axis=1,
        )
        turned = dot_split((left_ref[0], left_ref[1]), split(pair))
        for half in range(2):
            columns = slice(half * LANES, (half + 1) * LANES)
            upper, lower = turned[0:left_size, columns], turned[left_size:, columns]
            middle_real.append(upper * twist_real - lower * twist_imag)
            middle_imag.append(upper * twist_imag + lower * twist_real)
    stacked = jnp.concatenate(
        [jnp.concatenate(middle_real, axis=0), jnp.concatenate(middle_imag, axis=0)], axis=1
    )
    spectrum = dot_split(split(stacked), (right_ref[0], right_ref[1]))
    upper = spectrum[:, 0:LANES].reshape(bins, left_size, LANES)
    lower = spectrum[:, LANES:].reshape(bins, left_size, LANES)
    spec_real, spec_imag = spec_ref[0][None], spec_ref[1][None]
    stacked = jnp.concatenate(
        [
            (upper * spec_real - lower * spec_imag).reshape(bins * left_size, LANES),
            (upper * spec_imag + lower * spec_real).reshape(bins * left_size, LANES),
        ],
        axis=1,
    )
    stacked = dot_split(split(stacked), (right_ref[2], right_ref[3]))
    upper = stacked[:, 0:LANES].reshape(bins, left_size, LANES)
    lower = stacked[:, LANES:].reshape(bins, left_size, LANES)
    middle_real = upper * twist_real[None] + lower * twist_imag[None]
    middle_imag = lower * twist_real[None] - upper * twist_imag[None]
    result_real, result_imag = [], []
    for one in range(0, bins, 2):
        pair = jnp.concatenate(
            [
                jnp.concatenate([middle_real[one], middle_imag[one]], axis=0),
                jnp.concatenate([middle_real[one + 1], middle_imag[one + 1]], axis=0),
            ],
            axis=1,
        )
        turned = dot_split((left_ref[2], left_ref[3]), split(pair))
        for half in range(2):
            columns = slice(half * LANES, (half + 1) * LANES)
            result_real.append(turned[0:left_size, columns])
            result_imag.append(turned[left_size:, columns])
    return (
        jnp.stack(result_real).reshape(bins, lines),
        jnp.stack(result_imag).reshape(bins, lines),
    )


def first_kernel(in_ref, spec_ref, left_ref, right_ref, twist_ref, out_ref):
    out_ref[0], out_ref[1] = azimuth_image(in_ref, spec_ref, left_ref, right_ref, twist_ref)


def azimuth_box(values):
    rows, lines = values.shape
    values = jnp.concatenate([values, jnp.zeros((rows, LANES), jnp.float32)], axis=1)
    total = lines + LANES
    for step in (1, 2, 4):
        values = values + pltpu.roll(values, total - step, 1)
    return pltpu.roll(values, 3, 1)[:, 0:lines]


def second_kernel(
    shift_ref, in_ref, first_ref, spec_ref, left_ref, right_ref, twist_ref, out_ref
):
    real, imag = azimuth_image(in_ref, spec_ref, left_ref, right_ref, twist_ref)
    source = lax.broadcasted_iota(jnp.int32, real.shape, 1) - shift_ref[0]
    inside = (source >= 0) & (source < real.shape[1])
    real, imag = jnp.where(inside, real, 0.0), jnp.where(inside, imag, 0.0)
    first_real, first_imag = first_ref[0], first_ref[1]
    out_ref[0] = azimuth_box(first_real * real + first_imag * imag)
    out_ref[1] = azimuth_box(first_imag * real - first_real * imag)
    out_ref[2] = azimuth_box(first_real * first_real + first_imag * first_imag)
    out_ref[3] = azimuth_box(real * real + imag * imag)


def azimuth_call(ranged, spec, tabs, first=None, shift=None):
    left, right, twist = tabs
    parts, _, bins, lines_count = ranged.shape
    lines = parts * lines_count
    height = 8

    def whole(array):
        return pl.BlockSpec(array.shape, lambda i: (0,) * array.ndim)

    block = pl.BlockSpec((2, height, lines), lambda i: (0, i, 0))
    source = pl.BlockSpec((parts, 2, height, lines_count), lambda i: (0, 0, i, 0))
    operands, specs = [ranged], [source]
    if first is not None:
        operands = [shift, ranged, first]
        specs = [pl.BlockSpec(memory_space=pltpu.SMEM), source, block]
    constants = [spec, left, right, twist]
    outs = 2 if first is None else 4
    return pl.pallas_call(
        first_kernel if first is None else second_kernel,
        out_shape=jax.ShapeDtypeStruct((outs, bins, lines), jnp.float32),
        grid=(bins // height,),
        in_specs=specs + [whole(array) for array in constants],
        out_specs=pl.BlockSpec((outs, height, lines), lambda i: (0, i, 0)),
        compiler_params=pltpu.CompilerParams(vmem_limit_bytes=VMEM_BYTES),
        cost_estimate=pl.CostEstimate(
            flops=24 * 512 * bins * lines,
            bytes_accessed=4 * bins * lines * (2 + outs),
            transcendentals=0,
        ),
        name="azimuth_first" if first is None else "azimuth_second",
    )(*operands, *constants)


def range_box_kernel(sums_ref, low_ref, high_ref, inter_ref, coherence_ref, scratch):
    bins = sums_ref.shape[1]
    boxes = []
    for part in range(4):
        scratch[4:8, :] = low_ref[part]
        scratch[pl.ds(8, bins), :] = sums_ref[part]
        scratch[pl.ds(8 + bins, 4), :] = high_ref[part]
        values = scratch[pl.ds(5, bins + 7), :]
        values = values[:-1] + values[1:]
        values = values[:-2] + values[2:]
        boxes.append(values[:-4] + values[4:])
    inter_ref[0] = boxes[0] * (1.0 / 64.0)
    inter_ref[1] = boxes[1] * (1.0 / 64.0)
    coherence_ref[...] = jnp.sqrt(boxes[0] * boxes[0] + boxes[1] * boxes[1]) / jnp.sqrt(
        boxes[2] * boxes[3] + 1.0
    )


def range_box(sums, low, high):
    _, bins, lines = sums.shape
    width = 512
    return pl.pallas_call(
        range_box_kernel,
        out_shape=(
            jax.ShapeDtypeStruct((2, bins, lines), jnp.float32),
            jax.ShapeDtypeStruct((bins, lines), jnp.float32),
        ),
        grid=(lines // width,),
        in_specs=[
            pl.BlockSpec((4, bins, width), lambda i: (0, 0, i)),
            pl.BlockSpec((4, 4, width), lambda i: (0, 0, i)),
            pl.BlockSpec((4, 4, width), lambda i: (0, 0, i)),
        ],
        out_specs=(
            pl.BlockSpec((2, bins, width), lambda i: (0, 0, i)),
            pl.BlockSpec((bins, width), lambda i: (0, i)),
        ),
        scratch_shapes=[pltpu.VMEM((bins + 16, width), jnp.float32)],
        compiler_params=pltpu.CompilerParams(vmem_limit_bytes=VMEM_BYTES),
        name="range_box",
    )(sums, low, high)


def stacked_tables(real, imag, left):
    if left:
        real_form = jnp.concatenate(
            [jnp.concatenate([real, -imag], 1), jnp.concatenate([imag, real], 1)], 0
        )
    else:
        real_form = jnp.concatenate(
            [jnp.concatenate([real, imag], 1), jnp.concatenate([-imag, real], 1)], 0
        )
    high = lax.reduce_precision(real_form, 8, 7)
    return high.astype(jnp.bfloat16), (real_form - high).astype(jnp.bfloat16)


def neighbours(block, axis, width):
    count = lax.axis_size(axis)
    ahead = [(i, i + 1) for i in range(count - 1)]
    back = [(target, source) for source, target in ahead]
    return (
        lax.ppermute(block[:, -width:], axis, ahead),
        lax.ppermute(block[:, :width], axis, back),
    )


def staged_on_device(raw_first, raw_second, offsets, chirp_lengths):
    lines_count = raw_first.shape[1]
    range_count = raw_first.shape[2]
    azimuth_count = lines_count * lax.axis_size("az")
    longest = min(range_count, azimuth_count) // 4
    segments = chirp_segments(chirp_lengths[0], longest // TILE + 1)
    first_ranged = range_focus(raw_first, segments, offsets[1:2], False)
    second_ranged = range_focus(raw_second, segments, offsets[1:2], True)
    first_turned = lax.all_to_all(first_ranged, "az", split_axis=0, concat_axis=0, tiled=True)
    second_turned = lax.all_to_all(second_ranged, "az", split_axis=0, concat_axis=0, tiled=True)

    entries, left_size, right_size = tables(azimuth_count)
    left_real, left_imag, right_real, right_imag, twist_real, twist_imag = entries
    left = jnp.stack(
        stacked_tables(left_real, left_imag, True) + stacked_tables(left_real, -left_imag, True)
    )
    right = jnp.stack(
        stacked_tables(right_real, right_imag, False)
        + stacked_tables(right_real, -right_imag, False)
    )
    tabs = (left, right, jnp.stack([twist_real, twist_imag]))
    chirp_real, chirp_imag = chirp(chirp_lengths[1], azimuth_count)
    spec = forward(
        jnp.stack([chirp_real, chirp_imag]).reshape(2, 1, left_size, right_size),
        entries,
        along_forms,
    )[:, 0]
    spec = jnp.stack([spec[0], -spec[1]]) * (1.0 / azimuth_count)
    frequency = lax.broadcasted_iota(
        jnp.int32, (left_size, right_size), 0
    ) + left_size * lax.broadcasted_iota(jnp.int32, (left_size, right_size), 1)
    turns = jnp.mod(frequency * offsets[0], azimuth_count).astype(jnp.float32)
    angles = -2.0 * math.pi / azimuth_count * turns
    second_spec = complex_times(spec, jnp.cos(angles), jnp.sin(angles))

    first_image = azimuth_call(first_turned, spec, tabs)
    sums = azimuth_call(second_turned, second_spec, tabs, first_image, offsets[0:1])
    low, high = neighbours(sums, "az", 4)
    return range_box(sums, low, high)


ROWS = 8


def host_tables(lines):
    left_size, right_size = lines // LANES, LANES

    def turn(rows_count, cols_count, period):
        product = np.outer(np.arange(rows_count), np.arange(cols_count)) % period
        angles = -2.0 * np.pi / period * product
        return np.cos(angles), np.sin(angles)

    def stacked(real, imag, left):
        sign = -1.0 if left else 1.0
        form = np.block([[real, sign * imag], [-sign * imag, real]]).astype(np.float32)
        high = form.astype(jnp.bfloat16)
        low = (form - high.astype(np.float32)).astype(jnp.bfloat16)
        return [high, low]

    left_real, left_imag = turn(left_size, left_size, left_size)
    right_real, right_imag = turn(right_size, right_size, right_size)
    twist = turn(left_size, right_size, lines)
    left = np.stack(stacked(left_real, left_imag, True) + stacked(left_real, -left_imag, True))
    right = np.stack(
        stacked(right_real, right_imag, False) + stacked(right_real, -right_imag, False)
    )
    return jnp.asarray(left), jnp.asarray(right), jnp.asarray(np.stack(twist).astype(np.float32))


def chirp_values(sample, length):
    inside = (sample >= 0) & (sample < length)
    offset = 2 * jnp.clip(sample, 0, length) - length
    period = 8 * length
    square = offset * offset
    turns = jnp.floor(square.astype(jnp.float32) / period.astype(jnp.float32)).astype(jnp.int32)
    numerator = square - turns * period
    numerator = jnp.where(numerator < 0, numerator + period, numerator)
    numerator = jnp.where(numerator >= period, numerator - period, numerator)
    scale = length.astype(jnp.float32)
    angles = jnp.pi * numerator.astype(jnp.float32) / (4.0 * scale)
    amplitude = jnp.where(inside, 1.0 / jnp.sqrt(jnp.full(sample.shape, scale)), 0.0)
    return amplitude * jnp.cos(angles), amplitude * jnp.sin(angles)


def azimuth_filter(length, shift, lines, left_ref, right_ref, twist_ref, spec_ref):
    left_size = lines // LANES
    shape = (left_size, LANES)
    row, column = (lax.broadcasted_iota(jnp.int32, shape, axis) for axis in range(2))
    real, imag = chirp_values(row * LANES + column, length)
    turned = dot_split(
        (left_ref[0], left_ref[1]), split(jnp.concatenate([real, imag], axis=0))
    )
    upper, lower = turned[0:left_size], turned[left_size:]
    twist_real, twist_imag = twist_ref[0], twist_ref[1]
    stacked = jnp.concatenate(
        [upper * twist_real - lower * twist_imag, upper * twist_imag + lower * twist_real], axis=1
    )
    stacked = dot_split(split(stacked), (right_ref[0], right_ref[1])) * (1.0 / lines)
    real, imag = stacked[:, 0:LANES], -stacked[:, LANES:]
    spec_ref[0, 0], spec_ref[0, 1] = real, imag
    frequency = row + left_size * column
    turns = ((frequency * shift) & (lines - 1)).astype(jnp.float32)
    angles = (-2.0 * math.pi / lines) * turns
    turn_real, turn_imag = jnp.cos(angles), jnp.sin(angles)
    spec_ref[1, 0] = real * turn_real - imag * turn_imag
    spec_ref[1, 1] = real * turn_imag + imag * turn_real


def build_table(taps, lead, length, seg_ref, tab_ref):
    rows = seg_ref.shape[1]
    place = lax.broadcasted_iota(jnp.int32, (rows, 2 * TILE), 1)
    sample = lax.broadcasted_iota(jnp.int32, (rows, 2 * TILE), 0) * TILE - place
    sample = jnp.where(place < TILE, sample, sample + 2 * TILE) + lead
    real, imag = chirp_values(sample, length)
    seg_ref[0], seg_ref[1] = real, -imag

    def one(tap, carry):
        rows = pl.ds(pl.multiple_of(tap * TILE, TILE), TILE)
        for part in range(2):
            row = jnp.broadcast_to(seg_ref[part, pl.ds(tap, 1), :], (TILE, 2 * TILE))
            turned = pltpu.roll(row, 0, 1, stride=1, stride_axis=0)[:, 0:TILE]
            high, low = split(turned)
            columns, other = pl.ds(part * TILE, TILE), pl.ds((1 - part) * TILE, TILE)
            tab_ref[0, rows, columns] = high
            tab_ref[1, rows, columns] = low
            tab_ref[2, rows, other] = high if part == 0 else -high
            tab_ref[3, rows, other] = low if part == 0 else -low
        return carry

    lax.fori_loop(0, taps, one, 0)


def fused_kernel(
    parts, taps,
    offset_ref, length_ref, raw_first, raw_second, left_ref, right_ref, twist_ref,
    inter_ref, coherence_ref,
    raw, tab, seg, spec, sent_first, sent_second, got_first, got_second, image, sums,
    edge_sent, edge_got, inter_out, coherence_out,
    raw_sem, first_send, first_recv, second_send, second_recv, edge_send_sem, edge_recv_sem,
    out_sem,
):
    me = lax.axis_index("az")
    bins, lines_count = sent_first.shape[2], sent_first.shape[3]
    lines = parts * lines_count
    groups = bins // ROWS
    halves = lines_count // TILE
    blocks = WINDOW // TILE
    per_block = TILE // bins
    last = parts - 1

    def load(source):
        width = raw.shape[2] - LANES
        return pltpu.make_async_copy(
            source.at[:, :, pl.ds(0, width)], raw.at[:, :, pl.ds(LANES, width)], raw_sem.at[0]
        )

    load(raw_first).start()
    barrier = pltpu.get_barrier_semaphore()

    def greet(step, carry):
        pl.semaphore_signal(barrier, inc=1, device_id={"az": lax.rem(me + step, parts)})
        return carry

    lax.fori_loop(1, parts, greet, 0)
    raw[:, :, 0:LANES] = jnp.zeros((2, lines_count, LANES), jnp.bfloat16)
    build_table(taps, 0, length_ref[0], seg, tab)
    load(raw_first).wait()
    pl.semaphore_wait(barrier, parts - 1)

    half = me // (parts // 2)
    turn = lax.rem(me // per_block, blocks // 2)

    def block_of(step):
        side = lax.rem(half + 1 + step // (blocks // 2), 2)
        return side * (blocks // 2) + lax.rem(step + turn, blocks // 2)

    def correlate(block, piece, start, depth, target, low):
        rows = pl.ds(pl.multiple_of(piece * TILE, TILE), TILE)
        columns = pl.ds(pl.multiple_of(start + block * TILE, LANES), depth)
        real, imag = raw[0, rows, columns], raw[1, rows, columns]
        table = pl.ds(0, depth)
        result = (dot(real, tab[0, table]) + dot(imag, tab[2, table])) + (
            dot(real, tab[1, table]) + dot(imag, tab[3, table])
        )
        for part in range(2):
            turned = result[:, part * TILE : (part + 1) * TILE].T
            if low is not None:
                place = block * TILE + lax.broadcasted_iota(jnp.int32, (TILE, TILE), 0)
                turned = jnp.where(place >= low, turned, 0.0)
            turned = turned.reshape(per_block, bins, TILE)
            where = pl.ds(block * per_block, per_block)
            target[where, part, ROWS:bins, rows] = turned[:, 0 : bins - ROWS]
            target[where, part, 0:ROWS, rows] = turned[:, bins - ROWS : bins]

    def first_copy(piece, dest, source):
        rows = pl.ds(pl.multiple_of(piece * TILE, TILE), TILE)
        return pltpu.make_async_remote_copy(
            src_ref=sent_first.at[dest, :, :, rows],
            dst_ref=got_first.at[source, :, :, rows],
            send_sem=first_send.at[piece, dest],
            recv_sem=first_recv.at[piece, source],
            device_id={"az": dest},
        )

    def first_tile(step, carry):
        block, piece = block_of(step // halves), lax.rem(step, halves)
        correlate(block, piece, LANES, taps * TILE, sent_first, None)

        def send(item, inner):
            dest = block * per_block + lax.rem(item + me, per_block)

            @pl.when(dest != me)
            def _():
                first_copy(piece, dest, me).start()

            return inner

        lax.fori_loop(0, per_block, send, 0)
        return carry

    lax.fori_loop(0, blocks * halves, first_tile, 0)

    load(raw_second).start()
    build_table(taps + 1, offset_ref[1] - LANES, length_ref[0], seg, tab)
    load(raw_second).wait()

    def second_tile(step, carry):
        correlate(
            step // halves, lax.rem(step, halves), 0, (taps + 1) * TILE, sent_second,
            offset_ref[1],
        )
        return carry

    lax.fori_loop(0, blocks * halves, second_tile, 0)

    def second_copy(group, dest, source):
        rows = pl.ds(pl.multiple_of(group * ROWS, ROWS), ROWS)
        return pltpu.make_async_remote_copy(
            src_ref=sent_second.at[dest, :, rows, :],
            dst_ref=got_second.at[source, :, rows, :],
            send_sem=second_send.at[group, dest],
            recv_sem=second_recv.at[group, source],
            device_id={"az": dest},
        )

    def send_second(start, stop):
        def send(item, carry):
            group, step = start + item // last, 1 + lax.rem(item, last)
            second_copy(group, lax.rem(me + step, parts), me).start()
            return carry

        lax.fori_loop(0, (stop - start) * last, send, 0)

    early = groups // 2
    send_second(0, early)
    got_first[me] = sent_first[me]
    got_second[me] = sent_second[me]
    sums[:, 0:ROWS, :] = jnp.zeros((4, ROWS, lines), jnp.float32)
    sums[:, pl.ds(ROWS + bins, ROWS), :] = jnp.zeros((4, ROWS, lines), jnp.float32)
    azimuth_filter(length_ref[1], offset_ref[0], lines, left_ref, right_ref, twist_ref, spec)

    def first_arrived(item, carry):
        piece, source = item // last, lax.rem(me + 1 + lax.rem(item, last), parts)
        first_copy(piece, source, source).wait_recv()
        return carry

    lax.fori_loop(0, halves * last, first_arrived, 0)

    def first_group(group, carry):
        rows = pl.ds(pl.multiple_of(group * ROWS, ROWS), ROWS)
        real, imag = azimuth_image(
            got_first.at[:, :, rows, :], spec.at[0], left_ref, right_ref, twist_ref
        )
        image[0, rows, :] = real
        image[1, rows, :] = imag
        return carry

    lax.fori_loop(0, groups, first_group, 0)

    def edge_copy(side, dest):
        return pltpu.make_async_remote_copy(
            src_ref=edge_sent.at[side],
            dst_ref=edge_got.at[side],
            send_sem=edge_send_sem.at[side],
            recv_sem=edge_recv_sem.at[side],
            device_id={"az": dest},
        )

    def out_copies(group):
        rows = pl.ds(pl.multiple_of(group * ROWS, ROWS), ROWS)
        return (
            pltpu.make_async_copy(
                inter_out.at[:, rows, :], inter_ref.at[:, rows, :], out_sem.at[0, group]
            ),
            pltpu.make_async_copy(
                coherence_out.at[rows, :], coherence_ref.at[rows, :], out_sem.at[1, group]
            ),
        )

    width = 4 * LANES

    def finish(group):
        start = group * ROWS

        def piece(item, carry):
            columns = pl.ds(pl.multiple_of(item * width, width), width)
            boxes = []
            for part in range(4):
                held = sums[part, pl.ds(pl.multiple_of(start, ROWS), 3 * ROWS), columns]
                for step in (1, 2, 4):
                    held = held + pltpu.roll(held, 3 * ROWS - step, 0)
                boxes.append(pltpu.roll(held, 3 * ROWS - 5, 0)[0:ROWS])
            rows = pl.ds(pl.multiple_of(start, ROWS), ROWS)
            inter_out[0, rows, columns] = boxes[0] * (1.0 / 64.0)
            inter_out[1, rows, columns] = boxes[1] * (1.0 / 64.0)
            coherence_out[rows, columns] = jnp.sqrt(
                boxes[0] * boxes[0] + boxes[1] * boxes[1]
            ) / jnp.sqrt(boxes[2] * boxes[3] + 1.0)
            return carry

        lax.fori_loop(0, lines // width, piece, 0)
        for copy in out_copies(group):
            copy.start()

    def second_group(group, carry):
        def arrived(step, inner):
            source = lax.rem(me + step, parts)
            second_copy(group, source, source).wait_recv()
            return inner

        lax.fori_loop(1, parts, arrived, 0)
        rows = pl.ds(pl.multiple_of(group * ROWS, ROWS), ROWS)
        real, imag = azimuth_image(
            got_second.at[:, :, rows, :], spec.at[1], left_ref, right_ref, twist_ref
        )
        source = lax.broadcasted_iota(jnp.int32, real.shape, 1) - offset_ref[0]
        inside = (source >= 0) & (source < lines)
        real, imag = jnp.where(inside, real, 0.0), jnp.where(inside, imag, 0.0)
        first_real, first_imag = image[0, rows, :], image[1, rows, :]
        place = lax.rem(group + groups - 1, groups)
        held = pl.ds(pl.multiple_of(ROWS + place * ROWS, ROWS), ROWS)
        sums[0, held, :] = azimuth_box(first_real * real + first_imag * imag)
        sums[1, held, :] = azimuth_box(first_imag * real - first_real * imag)
        sums[2, held, :] = azimuth_box(first_real * first_real + first_imag * first_imag)
        sums[3, held, :] = azimuth_box(real * real + imag * imag)

        @pl.when(group == 0)
        def _():
            for part in range(4):
                edge_sent[0, 4 * part : 4 * part + 4, :] = sums[part, ROWS + bins - 4 : ROWS + bins]

            @pl.when(me < last)
            def _():
                edge_copy(0, me + 1).start()

        @pl.when(group == 1)
        def _():
            for part in range(4):
                edge_sent[1, 4 * part : 4 * part + 4, :] = sums[part, ROWS : ROWS + 4]

            @pl.when(me > 0)
            def _():
                edge_copy(1, me - 1).start()

            send_second(early, groups)

        @pl.when(group >= 3)
        def _():
            finish(group - 2)

        @pl.when(group == groups - 2)
        def _():
            @pl.when(me > 0)
            def _():
                edge_copy(0, me - 1).wait_recv()
                for part in range(4):
                    sums[part, 4:8, :] = edge_got[0, 4 * part : 4 * part + 4, :]

            @pl.when(me < last)
            def _():
                edge_copy(1, me + 1).wait_recv()
                for part in range(4):
                    sums[part, ROWS + bins : ROWS + bins + 4, :] = edge_got[
                        1, 4 * part : 4 * part + 4, :
                    ]

            finish(0)

        return carry

    lax.fori_loop(0, groups, second_group, 0)
    finish(groups - 2)
    finish(groups - 1)

    def first_left(item, carry):
        piece, dest = item // last, lax.rem(me + 1 + lax.rem(item, last), parts)
        first_copy(piece, dest, me).wait_send()
        return carry

    lax.fori_loop(0, halves * last, first_left, 0)

    def second_left(item, carry):
        group, dest = item // last, lax.rem(me + 1 + lax.rem(item, last), parts)
        second_copy(group, dest, me).wait_send()
        return carry

    lax.fori_loop(0, groups * last, second_left, 0)

    @pl.when(me < last)
    def _():
        edge_copy(0, me + 1).wait_send()

    @pl.when(me > 0)
    def _():
        edge_copy(1, me - 1).wait_send()

    def stored(group, carry):
        for copy in out_copies(group):
            copy.wait()
        return carry

    lax.fori_loop(0, groups, stored, 0)


def fits(parts, lines_count, range_count):
    lines = parts * lines_count
    bins = WINDOW // parts
    return (
        lines_count % TILE == 0
        and lines & (lines - 1) == 0
        and lines // LANES == LANES // 2
        and bins % ROWS == 0
        and bins >= 6 * ROWS
        and TILE % bins == 0
        and parts % 2 == 0
        and range_count >= WINDOW + (min(range_count, lines) // 4) + 2 * TILE
    )


def on_device(raw_first, raw_second, offsets, chirp_lengths):
    parts = lax.axis_size("az")
    lines_count, range_count = raw_first.shape[1:]
    if not fits(parts, lines_count, range_count):
        return staged_on_device(raw_first, raw_second, offsets, chirp_lengths)
    lines = parts * lines_count
    bins = WINDOW // parts
    groups, halves = bins // ROWS, lines_count // TILE
    taps = min(range_count, lines) // 4 // TILE + 1
    depth = (taps + 1) * TILE
    left, right, twist = host_tables(lines)
    vmem = pl.BlockSpec(memory_space=pltpu.VMEM)
    smem = pl.BlockSpec(memory_space=pltpu.SMEM)
    hbm = pl.BlockSpec(memory_space=pl.ANY)
    shared = pltpu.VMEM((parts, 2, bins, lines_count), jnp.float32)
    dma = pltpu.SemaphoreType.DMA
    return pl.pallas_call(
        functools.partial(fused_kernel, parts, taps),
        out_shape=(
            jax.ShapeDtypeStruct((2, bins, lines), jnp.float32),
            jax.ShapeDtypeStruct((bins, lines), jnp.float32),
        ),
        in_specs=[smem, smem, hbm, hbm, vmem, vmem, vmem],
        out_specs=(hbm, hbm),
        scratch_shapes=[
            pltpu.VMEM((2, lines_count, WINDOW - TILE + depth), jnp.bfloat16),
            pltpu.VMEM((4, depth, 2 * TILE), jnp.bfloat16),
            pltpu.VMEM((2, (taps + ROWS) // ROWS * ROWS, 2 * TILE), jnp.float32),
            pltpu.VMEM((2, 2, lines // LANES, LANES), jnp.float32),
            shared,
            shared,
            shared,
            shared,
            pltpu.VMEM((2, bins, lines), jnp.float32),
            pltpu.VMEM((4, bins + 2 * ROWS, lines), jnp.float32),
            pltpu.VMEM((2, 16, lines), jnp.float32),
            pltpu.VMEM((2, 16, lines), jnp.float32),
            pltpu.VMEM((2, bins, lines), jnp.float32),
            pltpu.VMEM((bins, lines), jnp.float32),
            dma((1,)),
            dma((halves, parts)),
            dma((halves, parts)),
            dma((groups, parts)),
            dma((groups, parts)),
            dma((2,)),
            dma((2,)),
            dma((2, groups)),
        ],
        compiler_params=pltpu.CompilerParams(
            collective_id=0, has_side_effects=True, vmem_limit_bytes=67043328
        ),
        name="fused",
    )(offsets, chirp_lengths, raw_first, raw_second, left, right, twist)


def solution(mesh):
    in_specs = (P("groups", "az", None), P("groups", "az", None), P("groups"), P("groups"))
    out_specs = (P("groups", "az", None), P(("groups", "az"), None))
    return jax.shard_map(
        on_device, mesh=mesh, in_specs=in_specs, out_specs=out_specs, check_vma=False
    )
```

```python
import functools
import math

import jax
import jax.numpy as jnp
import numpy as np
from jax import lax
from jax.experimental import pallas as pl
from jax.experimental.pallas import tpu as pltpu
from jax.sharding import PartitionSpec as P

WINDOW = 1024
MAXSHIFT = 16
LANES = 128
TILE = 256
VMEM_BYTES = 60 * 1024 * 1024


along_forms = (
    ("rij", "ik", "rkj"),
    ("rkj", "jl", "rkl"),
    ("rkl", "jl", "rkj"),
    ("rkj", "ik", "rij"),
)


def padded_2(block, sides, width):
    for axis, dim in sides:
        count = lax.axis_size(axis)
        forward = [(i, i + 1) for i in range(count - 1)]
        backward = [(target, source) for source, target in forward]
        low = lax.ppermute(
            lax.slice_in_dim(block, block.shape[dim] - width, None, axis=dim), axis, forward
        )
        high = lax.ppermute(lax.slice_in_dim(block, 0, width, axis=dim), axis, backward)
        block = jnp.concatenate([low, block, high], axis=dim)
    return block


def chirp(length, samples_all):
    sample = jnp.arange(samples_all, dtype=jnp.int32)
    offset = 2 * sample - length
    period = 8 * length
    numerator = jnp.mod(offset * offset, period)
    angles = jnp.pi * numerator.astype(jnp.float32) / (4 * length).astype(jnp.float32)
    amplitude = jnp.where(sample < length, 1.0 / jnp.sqrt(length.astype(jnp.float32)), 0.0)
    return (amplitude * jnp.cos(angles), amplitude * jnp.sin(angles))


def roots(rows_count, cols_count, period):
    product = lax.broadcasted_iota(jnp.int32, (rows_count, cols_count), 0) * lax.broadcasted_iota(
        jnp.int32, (rows_count, cols_count), 1
    )
    angles = -2.0 * math.pi / period * jnp.mod(product, period).astype(jnp.float32)
    return (jnp.cos(angles), jnp.sin(angles))


def tables(length):
    right_size = LANES
    left_size = length // right_size
    entries = (
        roots(left_size, left_size, left_size)
        + roots(right_size, right_size, right_size)
        + roots(left_size, right_size, length)
    )
    return (entries, left_size, right_size)


def complex_product(form, stacked, table_real, table_imag):
    left_side, right_side, result_side = form
    matrix = jnp.stack([jnp.stack([table_real, table_imag]), jnp.stack([-table_imag, table_real])])
    return jnp.einsum(
        "c" + left_side + ",cd" + right_side + "->d" + result_side,
        stacked,
        matrix,
        precision=lax.Precision.HIGHEST,
    )


def complex_times(stacked, other_real, other_imag):
    return jnp.stack(
        [
            stacked[0] * other_real - stacked[1] * other_imag,
            stacked[0] * other_imag + stacked[1] * other_real,
        ]
    )


def forward(stacked, entries, forms):
    left_real, left_imag, right_real, right_imag, twist_real, twist_imag = entries
    stacked = complex_product(forms[0], stacked, left_real, left_imag)
    stacked = complex_times(stacked, twist_real, twist_imag)
    return complex_product(forms[1], stacked, right_real, right_imag)


def split(values):
    high = values.astype(jnp.bfloat16)
    return high, (values - high.astype(jnp.float32)).astype(jnp.bfloat16)


def dot(left, right):
    return jnp.dot(left, right, preferred_element_type=jnp.float32)


def dot_split(left, right):
    return dot(left[0], right[0]) + (dot(left[0], right[1]) + dot(left[1], right[0]))


def chirp_segments(length, taps):
    place = lax.broadcasted_iota(jnp.int32, (taps, 2 * TILE), 1)
    sample = lax.broadcasted_iota(jnp.int32, (taps, 2 * TILE), 0) * TILE - place
    sample = jnp.where(place < TILE, sample, sample + 2 * TILE)
    offset = 2 * sample - length
    numerator = jnp.mod(offset * offset, 8 * length)
    angles = jnp.pi * numerator.astype(jnp.float32) / (4 * length).astype(jnp.float32)
    inside = (sample >= 0) & (sample < length)
    amplitude = jnp.where(inside, 1.0 / jnp.sqrt(length.astype(jnp.float32)), 0.0)
    return jnp.stack([amplitude * jnp.cos(angles), -amplitude * jnp.sin(angles)], axis=1)


def range_kernel(
    taps, shifted, shift_ref, seg_ref, raw_ref, out_ref, real_high, real_low, imag_high, imag_low,
    *rest,
):
    depth = taps * TILE

    @pl.when(pl.program_id(0) == 0)
    def _():
        for tap in range(taps):
            rows = pl.ds(tap * TILE, TILE)
            turned = []
            for part in range(2):
                row = jnp.broadcast_to(seg_ref[tap, pl.ds(part, 1), :], (TILE, 2 * TILE))
                turned.append(pltpu.roll(row, 0, 1, stride=1, stride_axis=0)[:, 0:TILE])
            for part, (columns, high_ref, low_ref) in enumerate(
                (
                    (0, real_high, real_low),
                    (TILE, real_high, real_low),
                )
            ):
                high, low = split(turned[part])
                high_ref[rows, pl.ds(columns, TILE)] = high
                low_ref[rows, pl.ds(columns, TILE)] = low
                if part == 0:
                    imag_high[rows, pl.ds(TILE, TILE)] = high
                    imag_low[rows, pl.ds(TILE, TILE)] = low
                else:
                    imag_high[rows, pl.ds(0, TILE)] = -high
                    imag_low[rows, pl.ds(0, TILE)] = -low
            if shifted:
                edge_real_high, edge_real_low, edge_imag_high, edge_imag_low = rest[1:]
                real, imag = turned[0][:, 0:LANES], turned[1][:, 0:LANES]
                low_half = lax.broadcasted_iota(jnp.int32, (TILE, LANES), 1) < LANES // 2
                high, low = split(jnp.where(low_half, real, pltpu.roll(imag, LANES // 2, 1)))
                edge_real_high[rows], edge_real_low[rows] = high, low
                high, low = split(jnp.where(low_half, -imag, pltpu.roll(real, LANES // 2, 1)))
                edge_imag_high[rows], edge_imag_low[rows] = high, low

    def correlated(start, tabs):
        columns = pl.ds(start, depth)
        real, imag = raw_ref[0, :, columns], raw_ref[1, :, columns]
        return (dot(real, tabs[0][...]) + dot(imag, tabs[2][...])) + (
            dot(real, tabs[1][...]) + dot(imag, tabs[3][...])
        )

    tabs = (real_high, real_low, imag_high, imag_low)
    bins = out_ref.shape[2]
    for block in range(WINDOW // TILE):
        result = correlated(block * TILE, tabs)
        for part in range(2):
            turned = result[:, part * TILE : (part + 1) * TILE].T
            if shifted:
                rest[0][part, pl.ds(MAXSHIFT + block * TILE, TILE), :] = turned
            else:
                out_ref[pl.ds(block * TILE // bins, TILE // bins), part] = turned.reshape(
                    TILE // bins, bins, turned.shape[1]
                )
    if shifted:
        target = rest[0]
        edge = correlated(WINDOW, rest[1:]).T
        for part in range(2):
            target[part, 0:MAXSHIFT, :] = jnp.zeros((MAXSHIFT, edge.shape[1]), jnp.float32)
            target[part, pl.ds(MAXSHIFT + WINDOW, MAXSHIFT), :] = edge[
                part * LANES // 2 : part * LANES // 2 + MAXSHIFT
            ]
        held = WINDOW + 2 * MAXSHIFT
        turn = lax.rem(held - MAXSHIFT + shift_ref[0], held)
        for part in range(2):
            moved = pltpu.roll(target[part], turn, 0)[0:WINDOW]
            out_ref[:, part] = moved.reshape(WINDOW // bins, bins, moved.shape[1])


def range_focus(raw, segments, shift, shifted):
    parts = lax.axis_size("az")
    bins = WINDOW // parts
    taps = segments.shape[0]
    depth = taps * TILE
    lines_count = raw.shape[1]
    height = min(TILE, lines_count)
    width = depth + WINDOW
    scratch = [pltpu.VMEM((depth, 2 * TILE), jnp.bfloat16)] * 4
    if shifted:
        scratch += [pltpu.VMEM((2, WINDOW + 2 * MAXSHIFT, height), jnp.float32)]
        scratch += [pltpu.VMEM((depth, LANES), jnp.bfloat16)] * 4
    return pl.pallas_call(
        functools.partial(range_kernel, taps, shifted),
        out_shape=jax.ShapeDtypeStruct((parts, 2, bins, lines_count), jnp.float32),
        grid=(lines_count // height,),
        in_specs=[
            pl.BlockSpec(memory_space=pltpu.SMEM),
            pl.BlockSpec((taps, 2, 2 * TILE), lambda i: (0, 0, 0)),
            pl.BlockSpec((2, height, width), lambda i: (0, i, 0)),
        ],
        out_specs=pl.BlockSpec((parts, 2, bins, height), lambda i: (0, 0, 0, i)),
        scratch_shapes=scratch,
        compiler_params=pltpu.CompilerParams(vmem_limit_bytes=VMEM_BYTES),
        cost_estimate=pl.CostEstimate(
            flops=16 * lines_count * depth * WINDOW,
            bytes_accessed=4 * lines_count * (width + 2 * WINDOW),
            transcendentals=0,
        ),
        name="range_second" if shifted else "range_first",
    )(shift, segments, raw)


def azimuth_image(in_ref, spec_ref, left_ref, right_ref, twist_ref):
    parts, _, bins, lines_count = in_ref.shape
    lines = parts * lines_count
    left_size = lines // LANES
    real, imag = (
        jnp.concatenate([in_ref[one, part] for one in range(parts)], axis=1).reshape(
            bins, left_size, LANES
        )
        for part in range(2)
    )
    twist_real, twist_imag = twist_ref[0], twist_ref[1]
    middle_real, middle_imag = [], []
    for one in range(0, bins, 2):
        pair = jnp.concatenate(
            [
                jnp.concatenate([real[one], imag[one]], axis=0),
                jnp.concatenate([real[one + 1], imag[one + 1]], axis=0),
            ],
            axis=1,
        )
        turned = dot_split((left_ref[0], left_ref[1]), split(pair))
        for half in range(2):
            columns = slice(half * LANES, (half + 1) * LANES)
            upper, lower = turned[0:left_size, columns], turned[left_size:, columns]
            middle_real.append(upper * twist_real - lower * twist_imag)
            middle_imag.append(upper * twist_imag + lower * twist_real)
    stacked = jnp.concatenate(
        [jnp.concatenate(middle_real, axis=0), jnp.concatenate(middle_imag, axis=0)], axis=1
    )
    spectrum = dot_split(split(stacked), (right_ref[0], right_ref[1]))
    upper = spectrum[:, 0:LANES].reshape(bins, left_size, LANES)
    lower = spectrum[:, LANES:].reshape(bins, left_size, LANES)
    spec_real, spec_imag = spec_ref[0][None], spec_ref[1][None]
    stacked = jnp.concatenate(
        [
            (upper * spec_real - lower * spec_imag).reshape(bins * left_size, LANES),
            (upper * spec_imag + lower * spec_real).reshape(bins * left_size, LANES),
        ],
        axis=1,
    )
    stacked = dot_split(split(stacked), (right_ref[2], right_ref[3]))
    upper = stacked[:, 0:LANES].reshape(bins, left_size, LANES)
    lower = stacked[:, LANES:].reshape(bins, left_size, LANES)
    middle_real = upper * twist_real[None] + lower * twist_imag[None]
    middle_imag = lower * twist_real[None] - upper * twist_imag[None]
    result_real, result_imag = [], []
    for one in range(0, bins, 2):
        pair = jnp.concatenate(
            [
                jnp.concatenate([middle_real[one], middle_imag[one]], axis=0),
                jnp.concatenate([middle_real[one + 1], middle_imag[one + 1]], axis=0),
            ],
            axis=1,
        )
        turned = dot_split((left_ref[2], left_ref[3]), split(pair))
        for half in range(2):
            columns = slice(half * LANES, (half + 1) * LANES)
            result_real.append(turned[0:left_size, columns])
            result_imag.append(turned[left_size:, columns])
    return (
        jnp.stack(result_real).reshape(bins, lines),
        jnp.stack(result_imag).reshape(bins, lines),
    )


def first_kernel(in_ref, spec_ref, left_ref, right_ref, twist_ref, out_ref):
    out_ref[0], out_ref[1] = azimuth_image(in_ref, spec_ref, left_ref, right_ref, twist_ref)


def azimuth_box(values):
    rows, lines = values.shape
    values = jnp.concatenate([values, jnp.zeros((rows, LANES), jnp.float32)], axis=1)
    total = lines + LANES
    for step in (1, 2, 4):
        values = values + pltpu.roll(values, total - step, 1)
    return pltpu.roll(values, 3, 1)[:, 0:lines]


def second_kernel(
    shift_ref, in_ref, first_ref, spec_ref, left_ref, right_ref, twist_ref, out_ref
):
    real, imag = azimuth_image(in_ref, spec_ref, left_ref, right_ref, twist_ref)
    source = lax.broadcasted_iota(jnp.int32, real.shape, 1) - shift_ref[0]
    inside = (source >= 0) & (source < real.shape[1])
    real, imag = jnp.where(inside, real, 0.0), jnp.where(inside, imag, 0.0)
    first_real, first_imag = first_ref[0], first_ref[1]
    out_ref[0] = azimuth_box(first_real * real + first_imag * imag)
    out_ref[1] = azimuth_box(first_imag * real - first_real * imag)
    out_ref[2] = azimuth_box(first_real * first_real + first_imag * first_imag)
    out_ref[3] = azimuth_box(real * real + imag * imag)


def azimuth_call(ranged, spec, tabs, first=None, shift=None):
    left, right, twist = tabs
    parts, _, bins, lines_count = ranged.shape
    lines = parts * lines_count
    height = 8

    def whole(array):
        return pl.BlockSpec(array.shape, lambda i: (0,) * array.ndim)

    block = pl.BlockSpec((2, height, lines), lambda i: (0, i, 0))
    source = pl.BlockSpec((parts, 2, height, lines_count), lambda i: (0, 0, i, 0))
    operands, specs = [ranged], [source]
    if first is not None:
        operands = [shift, ranged, first]
        specs = [pl.BlockSpec(memory_space=pltpu.SMEM), source, block]
    constants = [spec, left, right, twist]
    outs = 2 if first is None else 4
    return pl.pallas_call(
        first_kernel if first is None else second_kernel,
        out_shape=jax.ShapeDtypeStruct((outs, bins, lines), jnp.float32),
        grid=(bins // height,),
        in_specs=specs + [whole(array) for array in constants],
        out_specs=pl.BlockSpec((outs, height, lines), lambda i: (0, i, 0)),
        compiler_params=pltpu.CompilerParams(vmem_limit_bytes=VMEM_BYTES),
        cost_estimate=pl.CostEstimate(
            flops=24 * 512 * bins * lines,
            bytes_accessed=4 * bins * lines * (2 + outs),
            transcendentals=0,
        ),
        name="azimuth_first" if first is None else "azimuth_second",
    )(*operands, *constants)


def range_box_kernel(sums_ref, low_ref, high_ref, inter_ref, coherence_ref, scratch):
    bins = sums_ref.shape[1]
    boxes = []
    for part in range(4):
        scratch[4:8, :] = low_ref[part]
        scratch[pl.ds(8, bins), :] = sums_ref[part]
        scratch[pl.ds(8 + bins, 4), :] = high_ref[part]
        values = scratch[pl.ds(5, bins + 7), :]
        values = values[:-1] + values[1:]
        values = values[:-2] + values[2:]
        boxes.append(values[:-4] + values[4:])
    inter_ref[0] = boxes[0] * (1.0 / 64.0)
    inter_ref[1] = boxes[1] * (1.0 / 64.0)
    coherence_ref[...] = jnp.sqrt(boxes[0] * boxes[0] + boxes[1] * boxes[1]) / jnp.sqrt(
        boxes[2] * boxes[3] + 1.0
    )


def range_box(sums, low, high):
    _, bins, lines = sums.shape
    width = 512
    return pl.pallas_call(
        range_box_kernel,
        out_shape=(
            jax.ShapeDtypeStruct((2, bins, lines), jnp.float32),
            jax.ShapeDtypeStruct((bins, lines), jnp.float32),
        ),
        grid=(lines // width,),
        in_specs=[
            pl.BlockSpec((4, bins, width), lambda i: (0, 0, i)),
            pl.BlockSpec((4, 4, width), lambda i: (0, 0, i)),
            pl.BlockSpec((4, 4, width), lambda i: (0, 0, i)),
        ],
        out_specs=(
            pl.BlockSpec((2, bins, width), lambda i: (0, 0, i)),
            pl.BlockSpec((bins, width), lambda i: (0, i)),
        ),
        scratch_shapes=[pltpu.VMEM((bins + 16, width), jnp.float32)],
        compiler_params=pltpu.CompilerParams(vmem_limit_bytes=VMEM_BYTES),
        name="range_box",
    )(sums, low, high)


def stacked_tables(real, imag, left):
    if left:
        real_form = jnp.concatenate(
            [jnp.concatenate([real, -imag], 1), jnp.concatenate([imag, real], 1)], 0
        )
    else:
        real_form = jnp.concatenate(
            [jnp.concatenate([real, imag], 1), jnp.concatenate([-imag, real], 1)], 0
        )
    high = lax.reduce_precision(real_form, 8, 7)
    return high.astype(jnp.bfloat16), (real_form - high).astype(jnp.bfloat16)


def neighbours(block, axis, width):
    count = lax.axis_size(axis)
    ahead = [(i, i + 1) for i in range(count - 1)]
    back = [(target, source) for source, target in ahead]
    return (
        lax.ppermute(block[:, -width:], axis, ahead),
        lax.ppermute(block[:, :width], axis, back),
    )


def staged_on_device(raw_first, raw_second, offsets, chirp_lengths):
    lines_count = raw_first.shape[1]
    range_count = raw_first.shape[2]
    azimuth_count = lines_count * lax.axis_size("az")
    longest = min(range_count, azimuth_count) // 4
    segments = chirp_segments(chirp_lengths[0], longest // TILE + 1)
    first_ranged = range_focus(raw_first, segments, offsets[1:2], False)
    second_ranged = range_focus(raw_second, segments, offsets[1:2], True)
    first_turned = lax.all_to_all(first_ranged, "az", split_axis=0, concat_axis=0, tiled=True)
    second_turned = lax.all_to_all(second_ranged, "az", split_axis=0, concat_axis=0, tiled=True)

    entries, left_size, right_size = tables(azimuth_count)
    left_real, left_imag, right_real, right_imag, twist_real, twist_imag = entries
    left = jnp.stack(
        stacked_tables(left_real, left_imag, True) + stacked_tables(left_real, -left_imag, True)
    )
    right = jnp.stack(
        stacked_tables(right_real, right_imag, False)
        + stacked_tables(right_real, -right_imag, False)
    )
    tabs = (left, right, jnp.stack([twist_real, twist_imag]))
    chirp_real, chirp_imag = chirp(chirp_lengths[1], azimuth_count)
    spec = forward(
        jnp.stack([chirp_real, chirp_imag]).reshape(2, 1, left_size, right_size),
        entries,
        along_forms,
    )[:, 0]
    spec = jnp.stack([spec[0], -spec[1]]) * (1.0 / azimuth_count)
    frequency = lax.broadcasted_iota(
        jnp.int32, (left_size, right_size), 0
    ) + left_size * lax.broadcasted_iota(jnp.int32, (left_size, right_size), 1)
    turns = jnp.mod(frequency * offsets[0], azimuth_count).astype(jnp.float32)
    angles = -2.0 * math.pi / azimuth_count * turns
    second_spec = complex_times(spec, jnp.cos(angles), jnp.sin(angles))

    first_image = azimuth_call(first_turned, spec, tabs)
    sums = azimuth_call(second_turned, second_spec, tabs, first_image, offsets[0:1])
    low, high = neighbours(sums, "az", 4)
    return range_box(sums, low, high)


ROWS = 8


def host_tables(lines):
    left_size, right_size = lines // LANES, LANES

    def turn(rows_count, cols_count, period):
        product = np.outer(np.arange(rows_count), np.arange(cols_count)) % period
        angles = -2.0 * np.pi / period * product
        return np.cos(angles), np.sin(angles)

    def stacked(real, imag, left):
        sign = -1.0 if left else 1.0
        form = np.block([[real, sign * imag], [-sign * imag, real]]).astype(np.float32)
        high = form.astype(jnp.bfloat16)
        low = (form - high.astype(np.float32)).astype(jnp.bfloat16)
        return [high, low]

    left_real, left_imag = turn(left_size, left_size, left_size)
    right_real, right_imag = turn(right_size, right_size, right_size)
    twist = turn(left_size, right_size, lines)
    left = np.stack(stacked(left_real, left_imag, True) + stacked(left_real, -left_imag, True))
    right = np.stack(
        stacked(right_real, right_imag, False) + stacked(right_real, -right_imag, False)
    )
    return jnp.asarray(left), jnp.asarray(right), jnp.asarray(np.stack(twist).astype(np.float32))


def chirp_values(sample, length):
    inside = (sample >= 0) & (sample < length)
    offset = 2 * jnp.clip(sample, 0, length) - length
    period = 8 * length
    square = offset * offset
    turns = jnp.floor(square.astype(jnp.float32) / period.astype(jnp.float32)).astype(jnp.int32)
    numerator = square - turns * period
    numerator = jnp.where(numerator < 0, numerator + period, numerator)
    numerator = jnp.where(numerator >= period, numerator - period, numerator)
    scale = length.astype(jnp.float32)
    angles = jnp.pi * numerator.astype(jnp.float32) / (4.0 * scale)
    amplitude = jnp.where(inside, 1.0 / jnp.sqrt(jnp.full(sample.shape, scale)), 0.0)
    return amplitude * jnp.cos(angles), amplitude * jnp.sin(angles)


def azimuth_filter(length, shift, lines, left_ref, right_ref, twist_ref, spec_ref):
    left_size = lines // LANES
    shape = (left_size, LANES)
    row, column = (lax.broadcasted_iota(jnp.int32, shape, axis) for axis in range(2))
    real, imag = chirp_values(row * LANES + column, length)
    turned = dot_split(
        (left_ref[0], left_ref[1]), split(jnp.concatenate([real, imag], axis=0))
    )
    upper, lower = turned[0:left_size], turned[left_size:]
    twist_real, twist_imag = twist_ref[0], twist_ref[1]
    stacked = jnp.concatenate(
        [upper * twist_real - lower * twist_imag, upper * twist_imag + lower * twist_real], axis=1
    )
    stacked = dot_split(split(stacked), (right_ref[0], right_ref[1])) * (1.0 / lines)
    real, imag = stacked[:, 0:LANES], -stacked[:, LANES:]
    spec_ref[0, 0], spec_ref[0, 1] = real, imag
    frequency = row + left_size * column
    turns = ((frequency * shift) & (lines - 1)).astype(jnp.float32)
    angles = (-2.0 * math.pi / lines) * turns
    turn_real, turn_imag = jnp.cos(angles), jnp.sin(angles)
    spec_ref[1, 0] = real * turn_real - imag * turn_imag
    spec_ref[1, 1] = real * turn_imag + imag * turn_real


def build_table(taps, lead, length, seg_ref, tab_ref):
    rows = seg_ref.shape[1]
    place = lax.broadcasted_iota(jnp.int32, (rows, 2 * TILE), 1)
    sample = lax.broadcasted_iota(jnp.int32, (rows, 2 * TILE), 0) * TILE - place
    sample = jnp.where(place < TILE, sample, sample + 2 * TILE) + lead
    real, imag = chirp_values(sample, length)
    seg_ref[0], seg_ref[1] = real, -imag

    def one(tap, carry):
        rows = pl.ds(pl.multiple_of(tap * TILE, TILE), TILE)
        for part in range(2):
            row = jnp.broadcast_to(seg_ref[part, pl.ds(tap, 1), :], (TILE, 2 * TILE))
            turned = pltpu.roll(row, 0, 1, stride=1, stride_axis=0)[:, 0:TILE]
            high, low = split(turned)
            columns, other = pl.ds(part * TILE, TILE), pl.ds((1 - part) * TILE, TILE)
            tab_ref[0, rows, columns] = high
            tab_ref[1, rows, columns] = low
            tab_ref[2, rows, other] = high if part == 0 else -high
            tab_ref[3, rows, other] = low if part == 0 else -low
        return carry

    lax.fori_loop(0, taps, one, 0)


def fused_kernel(
    parts, taps,
    offset_ref, length_ref, raw_first, raw_second, left_ref, right_ref, twist_ref,
    inter_out, coherence_out,
    raw, tab, seg, spec, sent_first, sent_second, got_first, got_second, image, windows,
    running, outer, edge_sent, edge_got,
    raw_sem, first_send, first_recv, second_send, second_recv, halo_send, halo_recv,
    edge_send_sem, edge_recv_sem,
):
    me = lax.axis_index("az")
    bins, lines_count = sent_first.shape[2], sent_first.shape[3]
    lines = parts * lines_count
    groups = bins // ROWS
    halves = lines_count // TILE
    blocks = WINDOW // TILE
    per_block = TILE // bins
    last = parts - 1
    middle = parts // 2
    extra = jnp.where((me == middle) | (me == middle - 1), 1, 0)

    def load(source, piece):
        width = raw.shape[2] - LANES
        rows = pl.ds(pl.multiple_of(piece * TILE, TILE), TILE)
        return pltpu.make_async_copy(
            source.at[:, rows, pl.ds(0, width)],
            raw.at[:, rows, pl.ds(LANES, width)],
            raw_sem.at[piece],
        )

    for piece in range(halves):
        load(raw_first, piece).start()
    barrier = pltpu.get_barrier_semaphore()

    def greet(step, carry):
        pl.semaphore_signal(barrier, inc=1, device_id={"az": lax.rem(me + step, parts)})
        return carry

    lax.fori_loop(1, parts, greet, 0)
    raw[:, :, 0:LANES] = jnp.zeros((2, lines_count, LANES), jnp.bfloat16)
    build_table(taps, 0, length_ref[0], seg, tab)
    pl.semaphore_wait(barrier, parts - 1)

    half = me // (parts // 2)
    turn = lax.rem(me // per_block, blocks // 2)

    def block_of(step):
        side = lax.rem(half + 1 + step // (blocks // 2), 2)
        return side * (blocks // 2) + lax.rem(step + turn, blocks // 2)

    def correlate(block, piece, start, depth, target, low):
        rows = pl.ds(pl.multiple_of(piece * TILE, TILE), TILE)
        columns = pl.ds(pl.multiple_of(start + block * TILE, LANES), depth)
        real, imag = raw[0, rows, columns], raw[1, rows, columns]
        table = pl.ds(0, depth)
        result = (dot(real, tab[0, table]) + dot(imag, tab[2, table])) + (
            dot(real, tab[1, table]) + dot(imag, tab[3, table])
        )
        for part in range(2):
            turned = result[:, part * TILE : (part + 1) * TILE].T
            if low is not None:
                place = block * TILE + lax.broadcasted_iota(jnp.int32, (TILE, TILE), 0)
                turned = jnp.where(place >= low, turned, 0.0)
            turned = turned.reshape(per_block, bins, TILE)
            where = pl.ds(block * per_block, per_block)
            target[where, part, ROWS:bins, rows] = turned[:, 0 : bins - ROWS]
            target[where, part, 0:ROWS, rows] = turned[:, bins - ROWS : bins]

    def first_copy(piece, dest, source):
        rows = pl.ds(pl.multiple_of(piece * TILE, TILE), TILE)
        return pltpu.make_async_remote_copy(
            src_ref=sent_first.at[dest, :, :, rows],
            dst_ref=got_first.at[source, :, pl.ds(0, bins), rows],
            send_sem=first_send.at[piece, dest],
            recv_sem=first_recv.at[piece, source],
            device_id={"az": dest},
        )

    def first_tile(step, carry):
        block, piece = block_of(step // halves), lax.rem(step, halves)

        @pl.when(step < halves)
        def _():
            load(raw_first, piece).wait()

        correlate(block, piece, LANES, taps * TILE, sent_first, None)

        def send(item, inner):
            dest = block * per_block + lax.rem(item + me, per_block)

            @pl.when(dest != me)
            def _():
                first_copy(piece, dest, me).start()

            return inner

        lax.fori_loop(0, per_block, send, 0)
        return carry

    lax.fori_loop(0, blocks * halves, first_tile, 0)

    for piece in range(halves):
        load(raw_second, piece).start()

    def halo_copy(number, side, source):
        sent, got = ((sent_first, got_first), (sent_second, got_second))[number]
        owner, start, place = ((middle, ROWS, 0), (middle - 1, ROWS // 2, ROWS // 2))[side]
        return pltpu.make_async_remote_copy(
            src_ref=sent.at[owner, :, pl.ds(start, ROWS // 2), :],
            dst_ref=got.at[source, :, pl.ds(bins + place, ROWS // 2), :],
            send_sem=halo_send.at[number, side],
            recv_sem=halo_recv.at[number, source],
            device_id={"az": middle - 1 + side},
        )

    def send_halo(number):
        sent, got = ((sent_first, got_first), (sent_second, got_second))[number]
        for side in range(2):
            @pl.when(me != middle - 1 + side)
            def _():
                halo_copy(number, side, me).start()

        half_rows = ROWS // 2

        @pl.when(me == middle - 1)
        def _():
            got[me, :, bins : bins + half_rows, :] = sent[middle, :, ROWS : ROWS + half_rows, :]

        @pl.when(me == middle)
        def _():
            got[me, :, bins + half_rows : bins + ROWS, :] = sent[middle - 1, :, half_rows:ROWS, :]

    def halo_arrived(number):
        for side in range(2):
            @pl.when(me == middle - 1 + side)
            def _():
                def one(step, carry):
                    source = lax.rem(me + step, parts)
                    halo_copy(number, side, source).wait_recv()
                    return carry

                lax.fori_loop(1, parts, one, 0)

    def halo_left(number):
        for side in range(2):
            @pl.when(me != middle - 1 + side)
            def _():
                halo_copy(number, side, me).wait_send()

    send_halo(0)
    build_table(taps + 1, offset_ref[1] - LANES, length_ref[0], seg, tab)
    for piece in range(halves):
        load(raw_second, piece).wait()

    def second_tile(step, carry):
        correlate(
            step // halves, lax.rem(step, halves), 0, (taps + 1) * TILE, sent_second,
            offset_ref[1],
        )
        return carry

    lax.fori_loop(0, blocks * halves, second_tile, 0)

    def second_copy(group, dest, source):
        rows = pl.ds(pl.multiple_of(group * ROWS, ROWS), ROWS)
        return pltpu.make_async_remote_copy(
            src_ref=sent_second.at[dest, :, rows, :],
            dst_ref=got_second.at[source, :, rows, :],
            send_sem=second_send.at[group, dest],
            recv_sem=second_recv.at[group, source],
            device_id={"az": dest},
        )

    def send_second(start, stop):
        def send(item, carry):
            group, step = start + item // last, 1 + lax.rem(item, last)
            second_copy(group, lax.rem(me + step, parts), me).start()
            return carry

        lax.fori_loop(0, (stop - start) * last, send, 0)

    early = groups // 2
    send_halo(1)
    send_second(0, early)
    got_first[me, :, 0:bins, :] = sent_first[me]
    got_second[me, :, 0:bins, :] = sent_second[me]
    running[...] = jnp.zeros((4, ROWS, lines), jnp.float32)
    azimuth_filter(length_ref[1], offset_ref[0], lines, left_ref, right_ref, twist_ref, spec)

    def first_arrived(item, carry):
        piece, source = item // last, lax.rem(me + 1 + lax.rem(item, last), parts)
        first_copy(piece, source, source).wait_recv()
        return carry

    lax.fori_loop(0, halves * last, first_arrived, 0)
    halo_arrived(0)

    def first_group(group, carry):
        rows = pl.ds(pl.multiple_of(group * ROWS, ROWS), ROWS)
        real, imag = azimuth_image(
            got_first.at[:, :, rows, :], spec.at[0], left_ref, right_ref, twist_ref
        )
        image[0, rows, :] = real
        image[1, rows, :] = imag
        return carry

    lax.fori_loop(0, groups + extra, first_group, 0)

    def edge_copy(side, dest):
        return pltpu.make_async_remote_copy(
            src_ref=edge_sent.at[side],
            dst_ref=edge_got.at[side],
            send_sem=edge_send_sem.at[side],
            recv_sem=edge_recv_sem.at[side],
            device_id={"az": dest},
        )

    row = lax.broadcasted_iota(jnp.int32, (ROWS, lines), 0)

    def scans(values):
        before = jnp.where(row >= 1, pltpu.roll(values, 1, 0), 0.0)
        after = values
        for step in (1, 2, 4):
            before = before + jnp.where(row >= step, pltpu.roll(before, step, 0), 0.0)
            after = after + jnp.where(
                row < ROWS - step, pltpu.roll(after, ROWS - step, 0), 0.0
            )
        return before, after

    def band(group):
        return pl.ds(pl.multiple_of(group * ROWS, ROWS), ROWS)

    def finish(group):
        rows = band(group)
        later = lax.broadcasted_iota(jnp.int32, (ROWS, lines), 0) >= 5
        boxes = [
            pltpu.roll(
                jnp.where(later, windows[part, rows, :], windows[part, band(group + 1), :]), 3, 0
            )
            for part in range(4)
        ]
        inter_out[0, rows, :] = boxes[0] * (1.0 / 64.0)
        inter_out[1, rows, :] = boxes[1] * (1.0 / 64.0)
        coherence_out[rows, :] = jnp.sqrt(boxes[0] * boxes[0] + boxes[1] * boxes[1]) / jnp.sqrt(
            boxes[2] * boxes[3] + 1.0
        )

    def second_group(item, carry):
        group = lax.rem(item + groups + 1, groups + 1)

        @pl.when(item >= 0)
        def _():
            def arrived(step, inner):
                source = lax.rem(me + step, parts)
                second_copy(group, source, source).wait_recv()
                return inner

            lax.fori_loop(1, parts, arrived, 0)

        @pl.when(item < 0)
        def _():
            halo_arrived(1)

        rows = band(group)
        real, imag = azimuth_image(
            got_second.at[:, :, rows, :], spec.at[1], left_ref, right_ref, twist_ref
        )
        source = lax.broadcasted_iota(jnp.int32, real.shape, 1) - offset_ref[0]
        inside = (source >= 0) & (source < lines)
        real, imag = jnp.where(inside, real, 0.0), jnp.where(inside, imag, 0.0)
        first_real, first_imag = image[0, rows, :], image[1, rows, :]
        products = (
            first_real * real + first_imag * imag,
            first_imag * real - first_real * imag,
            first_real * first_real + first_imag * first_imag,
            real * real + imag * imag,
        )
        for part in range(4):
            before, after = scans(azimuth_box(products[part]))
            outer[0, part] = before
            outer[1, part] = after

        @pl.when(item < 0)
        def _():
            for part in range(4):
                low, high = 4 * part, 4 * part + 4

                @pl.when(me == middle)
                def _():
                    edge_got[0, low:high, :] = outer[1, part, 4:8, :]

                @pl.when(me != middle)
                def _():
                    edge_got[1, low:high, :] = outer[0, part, 1:5, :]

        @pl.when(item == 0)
        def _():
            for part in range(4):
                edge_sent[0, 4 * part : 4 * part + 4, :] = outer[1, part, 4:8, :]
                windows[part, bins - ROWS : bins, :] = outer[0, part]
                windows[part, bins : bins + ROWS, :] = outer[1, part]

            @pl.when((me < last) & (me != middle - 1))
            def _():
                edge_copy(0, me + 1).start()

        @pl.when(item >= 1)
        def _():
            for part in range(4):
                windows[part, band(item - 1), :] = running[part] + outer[0, part]
                running[part] = outer[1, part]

        @pl.when(item == 1)
        def _():
            for part in range(4):
                edge_sent[1, 4 * part : 4 * part + 4, :] = outer[0, part, 1:5, :]

            @pl.when((me > 0) & (me != middle))
            def _():
                edge_copy(1, me - 1).start()

            send_second(early, groups)

        @pl.when(item >= 3)
        def _():
            finish(item - 2)

        @pl.when(item == groups - 2)
        def _():
            @pl.when(me > 0)
            def _():
                @pl.when(me != middle)
                def _():
                    edge_copy(0, me - 1).wait_recv()

                for part in range(4):
                    windows[part, 4:8, :] += edge_got[0, 4 * part : 4 * part + 4, :]

            @pl.when(me < last)
            def _():
                @pl.when(me != middle - 1)
                def _():
                    edge_copy(1, me + 1).wait_recv()

                for part in range(4):
                    windows[part, bins + 1 : bins + 5, :] += edge_got[
                        1, 4 * part : 4 * part + 4, :
                    ]

            finish(0)

        return carry

    lax.fori_loop(0 - extra, groups, second_group, 0)
    for part in range(4):
        windows[part, bins - ROWS : bins, :] += running[part]
    finish(groups - 2)
    finish(groups - 1)

    def first_left(item, carry):
        piece, dest = item // last, lax.rem(me + 1 + lax.rem(item, last), parts)
        first_copy(piece, dest, me).wait_send()
        return carry

    lax.fori_loop(0, halves * last, first_left, 0)

    def second_left(item, carry):
        group, dest = item // last, lax.rem(me + 1 + lax.rem(item, last), parts)
        second_copy(group, dest, me).wait_send()
        return carry

    lax.fori_loop(0, groups * last, second_left, 0)

    halo_left(0)
    halo_left(1)

    @pl.when((me < last) & (me != middle - 1))
    def _():
        edge_copy(0, me + 1).wait_send()

    @pl.when((me > 0) & (me != middle))
    def _():
        edge_copy(1, me - 1).wait_send()


def store_kernel(inter_ref, coherence_ref, inter_out, coherence_out, sems):
    copies = [
        pltpu.make_async_copy(inter_ref, inter_out, sems.at[0]),
        pltpu.make_async_copy(coherence_ref, coherence_out, sems.at[1]),
    ]
    for copy in copies:
        copy.start()
    for copy in copies:
        copy.wait()


def fits(parts, lines_count, range_count):
    lines = parts * lines_count
    bins = WINDOW // parts
    return (
        lines_count % TILE == 0
        and lines & (lines - 1) == 0
        and lines // LANES == LANES // 2
        and bins % ROWS == 0
        and bins >= 6 * ROWS
        and TILE % bins == 0
        and parts % 2 == 0
        and range_count >= WINDOW + (min(range_count, lines) // 4) + 2 * TILE
    )


def on_device(raw_first, raw_second, offsets, chirp_lengths):
    parts = lax.axis_size("az")
    lines_count, range_count = raw_first.shape[1:]
    if not fits(parts, lines_count, range_count):
        return staged_on_device(raw_first, raw_second, offsets, chirp_lengths)
    lines = parts * lines_count
    bins = WINDOW // parts
    groups, halves = bins // ROWS, lines_count // TILE
    taps = min(range_count, lines) // 4 // TILE + 1
    depth = (taps + 1) * TILE
    left, right, twist = host_tables(lines)
    vmem = pl.BlockSpec(memory_space=pltpu.VMEM)
    smem = pl.BlockSpec(memory_space=pltpu.SMEM)
    hbm = pl.BlockSpec(memory_space=pl.ANY)
    sent = pltpu.VMEM((parts, 2, bins, lines_count), jnp.float32)
    got = pltpu.VMEM((parts, 2, bins + ROWS, lines_count), jnp.float32)
    dma = pltpu.SemaphoreType.DMA
    held = pl.pallas_call(
        functools.partial(fused_kernel, parts, taps),
        out_shape=(
            pltpu.VMEM((2, bins, lines), jnp.float32),
            pltpu.VMEM((bins, lines), jnp.float32),
        ),
        in_specs=[smem, smem, hbm, hbm, vmem, vmem, vmem],
        out_specs=(vmem, vmem),
        scratch_shapes=[
            pltpu.VMEM((2, lines_count, WINDOW - TILE + depth), jnp.bfloat16),
            pltpu.VMEM((4, depth, 2 * TILE), jnp.bfloat16),
            pltpu.VMEM((2, (taps + ROWS) // ROWS * ROWS, 2 * TILE), jnp.float32),
            pltpu.VMEM((2, 2, lines // LANES, LANES), jnp.float32),
            sent,
            sent,
            got,
            got,
            pltpu.VMEM((2, bins + ROWS, lines), jnp.float32),
            pltpu.VMEM((4, bins + ROWS, lines), jnp.float32),
            pltpu.VMEM((4, ROWS, lines), jnp.float32),
            pltpu.VMEM((2, 4, ROWS, lines), jnp.float32),
            pltpu.VMEM((2, 16, lines), jnp.float32),
            pltpu.VMEM((2, 16, lines), jnp.float32),
            dma((halves,)),
            dma((halves, parts)),
            dma((halves, parts)),
            dma((groups, parts)),
            dma((groups, parts)),
            dma((2, 2)),
            dma((2, parts)),
            dma((2,)),
            dma((2,)),
        ],
        compiler_params=pltpu.CompilerParams(
            collective_id=0, has_side_effects=True, vmem_limit_bytes=57 * 1024 * 1024
        ),
        name="fused",
    )(offsets, chirp_lengths, raw_first, raw_second, left, right, twist)
    return pl.pallas_call(
        store_kernel,
        out_shape=(
            jax.ShapeDtypeStruct((2, bins, lines), jnp.float32),
            jax.ShapeDtypeStruct((bins, lines), jnp.float32),
        ),
        in_specs=[vmem, vmem],
        out_specs=(hbm, hbm),
        scratch_shapes=[dma((2,))],
        compiler_params=pltpu.CompilerParams(vmem_limit_bytes=1024 * 1024),
        name="store",
    )(*held)


def solution(mesh):
    in_specs = (P("groups", "az", None), P("groups", "az", None), P("groups"), P("groups"))
    out_specs = (P("groups", "az", None), P(("groups", "az"), None))
    return jax.shard_map(
        on_device, mesh=mesh, in_specs=in_specs, out_specs=out_specs, check_vma=False
    )
```

```python
import functools
import math

import jax
import jax.numpy as jnp
import numpy as np
from jax import lax
from jax.experimental import pallas as pl
from jax.experimental.pallas import tpu as pltpu
from jax.sharding import PartitionSpec as P

WINDOW = 1024
MAXSHIFT = 16
LANES = 128
TILE = 256
VMEM_BYTES = 60 * 1024 * 1024


along_forms = (
    ("rij", "ik", "rkj"),
    ("rkj", "jl", "rkl"),
    ("rkl", "jl", "rkj"),
    ("rkj", "ik", "rij"),
)


def padded_2(block, sides, width):
    for axis, dim in sides:
        count = lax.axis_size(axis)
        forward = [(i, i + 1) for i in range(count - 1)]
        backward = [(target, source) for source, target in forward]
        low = lax.ppermute(
            lax.slice_in_dim(block, block.shape[dim] - width, None, axis=dim), axis, forward
        )
        high = lax.ppermute(lax.slice_in_dim(block, 0, width, axis=dim), axis, backward)
        block = jnp.concatenate([low, block, high], axis=dim)
    return block


def chirp(length, samples_all):
    sample = jnp.arange(samples_all, dtype=jnp.int32)
    offset = 2 * sample - length
    period = 8 * length
    numerator = jnp.mod(offset * offset, period)
    angles = jnp.pi * numerator.astype(jnp.float32) / (4 * length).astype(jnp.float32)
    amplitude = jnp.where(sample < length, 1.0 / jnp.sqrt(length.astype(jnp.float32)), 0.0)
    return (amplitude * jnp.cos(angles), amplitude * jnp.sin(angles))


def roots(rows_count, cols_count, period):
    product = lax.broadcasted_iota(jnp.int32, (rows_count, cols_count), 0) * lax.broadcasted_iota(
        jnp.int32, (rows_count, cols_count), 1
    )
    angles = -2.0 * math.pi / period * jnp.mod(product, period).astype(jnp.float32)
    return (jnp.cos(angles), jnp.sin(angles))


def tables(length):
    right_size = LANES
    left_size = length // right_size
    entries = (
        roots(left_size, left_size, left_size)
        + roots(right_size, right_size, right_size)
        + roots(left_size, right_size, length)
    )
    return (entries, left_size, right_size)


def complex_product(form, stacked, table_real, table_imag):
    left_side, right_side, result_side = form
    matrix = jnp.stack([jnp.stack([table_real, table_imag]), jnp.stack([-table_imag, table_real])])
    return jnp.einsum(
        "c" + left_side + ",cd" + right_side + "->d" + result_side,
        stacked,
        matrix,
        precision=lax.Precision.HIGHEST,
    )


def complex_times(stacked, other_real, other_imag):
    return jnp.stack(
        [
            stacked[0] * other_real - stacked[1] * other_imag,
            stacked[0] * other_imag + stacked[1] * other_real,
        ]
    )


def forward(stacked, entries, forms):
    left_real, left_imag, right_real, right_imag, twist_real, twist_imag = entries
    stacked = complex_product(forms[0], stacked, left_real, left_imag)
    stacked = complex_times(stacked, twist_real, twist_imag)
    return complex_product(forms[1], stacked, right_real, right_imag)


def split(values):
    high = values.astype(jnp.bfloat16)
    return high, (values - high.astype(jnp.float32)).astype(jnp.bfloat16)


def dot(left, right):
    return jnp.dot(left, right, preferred_element_type=jnp.float32)


def dot_split(left, right):
    return dot(left[0], right[0]) + (dot(left[0], right[1]) + dot(left[1], right[0]))


def chirp_segments(length, taps):
    place = lax.broadcasted_iota(jnp.int32, (taps, 2 * TILE), 1)
    sample = lax.broadcasted_iota(jnp.int32, (taps, 2 * TILE), 0) * TILE - place
    sample = jnp.where(place < TILE, sample, sample + 2 * TILE)
    offset = 2 * sample - length
    numerator = jnp.mod(offset * offset, 8 * length)
    angles = jnp.pi * numerator.astype(jnp.float32) / (4 * length).astype(jnp.float32)
    inside = (sample >= 0) & (sample < length)
    amplitude = jnp.where(inside, 1.0 / jnp.sqrt(length.astype(jnp.float32)), 0.0)
    return jnp.stack([amplitude * jnp.cos(angles), -amplitude * jnp.sin(angles)], axis=1)


def range_kernel(
    taps, shifted, shift_ref, seg_ref, raw_ref, out_ref, real_high, real_low, imag_high, imag_low,
    *rest,
):
    depth = taps * TILE

    @pl.when(pl.program_id(0) == 0)
    def _():
        for tap in range(taps):
            rows = pl.ds(tap * TILE, TILE)
            turned = []
            for part in range(2):
                row = jnp.broadcast_to(seg_ref[tap, pl.ds(part, 1), :], (TILE, 2 * TILE))
                turned.append(pltpu.roll(row, 0, 1, stride=1, stride_axis=0)[:, 0:TILE])
            for part, (columns, high_ref, low_ref) in enumerate(
                (
                    (0, real_high, real_low),
                    (TILE, real_high, real_low),
                )
            ):
                high, low = split(turned[part])
                high_ref[rows, pl.ds(columns, TILE)] = high
                low_ref[rows, pl.ds(columns, TILE)] = low
                if part == 0:
                    imag_high[rows, pl.ds(TILE, TILE)] = high
                    imag_low[rows, pl.ds(TILE, TILE)] = low
                else:
                    imag_high[rows, pl.ds(0, TILE)] = -high
                    imag_low[rows, pl.ds(0, TILE)] = -low
            if shifted:
                edge_real_high, edge_real_low, edge_imag_high, edge_imag_low = rest[1:]
                real, imag = turned[0][:, 0:LANES], turned[1][:, 0:LANES]
                low_half = lax.broadcasted_iota(jnp.int32, (TILE, LANES), 1) < LANES // 2
                high, low = split(jnp.where(low_half, real, pltpu.roll(imag, LANES // 2, 1)))
                edge_real_high[rows], edge_real_low[rows] = high, low
                high, low = split(jnp.where(low_half, -imag, pltpu.roll(real, LANES // 2, 1)))
                edge_imag_high[rows], edge_imag_low[rows] = high, low

    def correlated(start, tabs):
        columns = pl.ds(start, depth)
        real, imag = raw_ref[0, :, columns], raw_ref[1, :, columns]
        return (dot(real, tabs[0][...]) + dot(imag, tabs[2][...])) + (
            dot(real, tabs[1][...]) + dot(imag, tabs[3][...])
        )

    tabs = (real_high, real_low, imag_high, imag_low)
    bins = out_ref.shape[2]
    for block in range(WINDOW // TILE):
        result = correlated(block * TILE, tabs)
        for part in range(2):
            turned = result[:, part * TILE : (part + 1) * TILE].T
            if shifted:
                rest[0][part, pl.ds(MAXSHIFT + block * TILE, TILE), :] = turned
            else:
                out_ref[pl.ds(block * TILE // bins, TILE // bins), part] = turned.reshape(
                    TILE // bins, bins, turned.shape[1]
                )
    if shifted:
        target = rest[0]
        edge = correlated(WINDOW, rest[1:]).T
        for part in range(2):
            target[part, 0:MAXSHIFT, :] = jnp.zeros((MAXSHIFT, edge.shape[1]), jnp.float32)
            target[part, pl.ds(MAXSHIFT + WINDOW, MAXSHIFT), :] = edge[
                part * LANES // 2 : part * LANES // 2 + MAXSHIFT
            ]
        held = WINDOW + 2 * MAXSHIFT
        turn = lax.rem(held - MAXSHIFT + shift_ref[0], held)
        for part in range(2):
            moved = pltpu.roll(target[part], turn, 0)[0:WINDOW]
            out_ref[:, part] = moved.reshape(WINDOW // bins, bins, moved.shape[1])


def range_focus(raw, segments, shift, shifted):
    parts = lax.axis_size("az")
    bins = WINDOW // parts
    taps = segments.shape[0]
    depth = taps * TILE
    lines_count = raw.shape[1]
    height = min(TILE, lines_count)
    width = depth + WINDOW
    scratch = [pltpu.VMEM((depth, 2 * TILE), jnp.bfloat16)] * 4
    if shifted:
        scratch += [pltpu.VMEM((2, WINDOW + 2 * MAXSHIFT, height), jnp.float32)]
        scratch += [pltpu.VMEM((depth, LANES), jnp.bfloat16)] * 4
    return pl.pallas_call(
        functools.partial(range_kernel, taps, shifted),
        out_shape=jax.ShapeDtypeStruct((parts, 2, bins, lines_count), jnp.float32),
        grid=(lines_count // height,),
        in_specs=[
            pl.BlockSpec(memory_space=pltpu.SMEM),
            pl.BlockSpec((taps, 2, 2 * TILE), lambda i: (0, 0, 0)),
            pl.BlockSpec((2, height, width), lambda i: (0, i, 0)),
        ],
        out_specs=pl.BlockSpec((parts, 2, bins, height), lambda i: (0, 0, 0, i)),
        scratch_shapes=scratch,
        compiler_params=pltpu.CompilerParams(vmem_limit_bytes=VMEM_BYTES),
        cost_estimate=pl.CostEstimate(
            flops=16 * lines_count * depth * WINDOW,
            bytes_accessed=4 * lines_count * (width + 2 * WINDOW),
            transcendentals=0,
        ),
        name="range_second" if shifted else "range_first",
    )(shift, segments, raw)


def azimuth_image(in_ref, spec_ref, left_ref, right_ref, twist_ref):
    parts, _, bins, lines_count = in_ref.shape
    lines = parts * lines_count
    left_size = lines // LANES
    real, imag = (
        jnp.concatenate([in_ref[one, part] for one in range(parts)], axis=1).reshape(
            bins, left_size, LANES
        )
        for part in range(2)
    )
    twist_real, twist_imag = twist_ref[0], twist_ref[1]
    middle_real, middle_imag = [], []
    for one in range(0, bins, 2):
        pair = jnp.concatenate(
            [
                jnp.concatenate([real[one], imag[one]], axis=0),
                jnp.concatenate([real[one + 1], imag[one + 1]], axis=0),
            ],
            axis=1,
        )
        turned = dot_split((left_ref[0], left_ref[1]), split(pair))
        for half in range(2):
            columns = slice(half * LANES, (half + 1) * LANES)
            upper, lower = turned[0:left_size, columns], turned[left_size:, columns]
            middle_real.append(upper * twist_real - lower * twist_imag)
            middle_imag.append(upper * twist_imag + lower * twist_real)
    stacked = jnp.concatenate(
        [jnp.concatenate(middle_real, axis=0), jnp.concatenate(middle_imag, axis=0)], axis=1
    )
    spectrum = dot_split(split(stacked), (right_ref[0], right_ref[1]))
    upper = spectrum[:, 0:LANES].reshape(bins, left_size, LANES)
    lower = spectrum[:, LANES:].reshape(bins, left_size, LANES)
    spec_real, spec_imag = spec_ref[0][None], spec_ref[1][None]
    stacked = jnp.concatenate(
        [
            (upper * spec_real - lower * spec_imag).reshape(bins * left_size, LANES),
            (upper * spec_imag + lower * spec_real).reshape(bins * left_size, LANES),
        ],
        axis=1,
    )
    stacked = dot_split(split(stacked), (right_ref[2], right_ref[3]))
    upper = stacked[:, 0:LANES].reshape(bins, left_size, LANES)
    lower = stacked[:, LANES:].reshape(bins, left_size, LANES)
    middle_real = upper * twist_real[None] + lower * twist_imag[None]
    middle_imag = lower * twist_real[None] - upper * twist_imag[None]
    result_real, result_imag = [], []
    for one in range(0, bins, 2):
        pair = jnp.concatenate(
            [
                jnp.concatenate([middle_real[one], middle_imag[one]], axis=0),
                jnp.concatenate([middle_real[one + 1], middle_imag[one + 1]], axis=0),
            ],
            axis=1,
        )
        turned = dot_split((left_ref[2], left_ref[3]), split(pair))
        for half in range(2):
            columns = slice(half * LANES, (half + 1) * LANES)
            result_real.append(turned[0:left_size, columns])
            result_imag.append(turned[left_size:, columns])
    return (
        jnp.stack(result_real).reshape(bins, lines),
        jnp.stack(result_imag).reshape(bins, lines),
    )


def first_kernel(in_ref, spec_ref, left_ref, right_ref, twist_ref, out_ref):
    out_ref[0], out_ref[1] = azimuth_image(in_ref, spec_ref, left_ref, right_ref, twist_ref)


def azimuth_box(values):
    rows, lines = values.shape
    values = jnp.concatenate([values, jnp.zeros((rows, LANES), jnp.float32)], axis=1)
    total = lines + LANES
    for step in (1, 2, 4):
        values = values + pltpu.roll(values, total - step, 1)
    return pltpu.roll(values, 3, 1)[:, 0:lines]


def second_kernel(
    shift_ref, in_ref, first_ref, spec_ref, left_ref, right_ref, twist_ref, out_ref
):
    real, imag = azimuth_image(in_ref, spec_ref, left_ref, right_ref, twist_ref)
    source = lax.broadcasted_iota(jnp.int32, real.shape, 1) - shift_ref[0]
    inside = (source >= 0) & (source < real.shape[1])
    real, imag = jnp.where(inside, real, 0.0), jnp.where(inside, imag, 0.0)
    first_real, first_imag = first_ref[0], first_ref[1]
    out_ref[0] = azimuth_box(first_real * real + first_imag * imag)
    out_ref[1] = azimuth_box(first_imag * real - first_real * imag)
    out_ref[2] = azimuth_box(first_real * first_real + first_imag * first_imag)
    out_ref[3] = azimuth_box(real * real + imag * imag)


def azimuth_call(ranged, spec, tabs, first=None, shift=None):
    left, right, twist = tabs
    parts, _, bins, lines_count = ranged.shape
    lines = parts * lines_count
    height = 8

    def whole(array):
        return pl.BlockSpec(array.shape, lambda i: (0,) * array.ndim)

    block = pl.BlockSpec((2, height, lines), lambda i: (0, i, 0))
    source = pl.BlockSpec((parts, 2, height, lines_count), lambda i: (0, 0, i, 0))
    operands, specs = [ranged], [source]
    if first is not None:
        operands = [shift, ranged, first]
        specs = [pl.BlockSpec(memory_space=pltpu.SMEM), source, block]
    constants = [spec, left, right, twist]
    outs = 2 if first is None else 4
    return pl.pallas_call(
        first_kernel if first is None else second_kernel,
        out_shape=jax.ShapeDtypeStruct((outs, bins, lines), jnp.float32),
        grid=(bins // height,),
        in_specs=specs + [whole(array) for array in constants],
        out_specs=pl.BlockSpec((outs, height, lines), lambda i: (0, i, 0)),
        compiler_params=pltpu.CompilerParams(vmem_limit_bytes=VMEM_BYTES),
        cost_estimate=pl.CostEstimate(
            flops=24 * 512 * bins * lines,
            bytes_accessed=4 * bins * lines * (2 + outs),
            transcendentals=0,
        ),
        name="azimuth_first" if first is None else "azimuth_second",
    )(*operands, *constants)


def range_box_kernel(sums_ref, low_ref, high_ref, inter_ref, coherence_ref, scratch):
    bins = sums_ref.shape[1]
    boxes = []
    for part in range(4):
        scratch[4:8, :] = low_ref[part]
        scratch[pl.ds(8, bins), :] = sums_ref[part]
        scratch[pl.ds(8 + bins, 4), :] = high_ref[part]
        values = scratch[pl.ds(5, bins + 7), :]
        values = values[:-1] + values[1:]
        values = values[:-2] + values[2:]
        boxes.append(values[:-4] + values[4:])
    inter_ref[0] = boxes[0] * (1.0 / 64.0)
    inter_ref[1] = boxes[1] * (1.0 / 64.0)
    coherence_ref[...] = jnp.sqrt(boxes[0] * boxes[0] + boxes[1] * boxes[1]) / jnp.sqrt(
        boxes[2] * boxes[3] + 1.0
    )


def range_box(sums, low, high):
    _, bins, lines = sums.shape
    width = 512
    return pl.pallas_call(
        range_box_kernel,
        out_shape=(
            jax.ShapeDtypeStruct((2, bins, lines), jnp.float32),
            jax.ShapeDtypeStruct((bins, lines), jnp.float32),
        ),
        grid=(lines // width,),
        in_specs=[
            pl.BlockSpec((4, bins, width), lambda i: (0, 0, i)),
            pl.BlockSpec((4, 4, width), lambda i: (0, 0, i)),
            pl.BlockSpec((4, 4, width), lambda i: (0, 0, i)),
        ],
        out_specs=(
            pl.BlockSpec((2, bins, width), lambda i: (0, 0, i)),
            pl.BlockSpec((bins, width), lambda i: (0, i)),
        ),
        scratch_shapes=[pltpu.VMEM((bins + 16, width), jnp.float32)],
        compiler_params=pltpu.CompilerParams(vmem_limit_bytes=VMEM_BYTES),
        name="range_box",
    )(sums, low, high)


def stacked_tables(real, imag, left):
    if left:
        real_form = jnp.concatenate(
            [jnp.concatenate([real, -imag], 1), jnp.concatenate([imag, real], 1)], 0
        )
    else:
        real_form = jnp.concatenate(
            [jnp.concatenate([real, imag], 1), jnp.concatenate([-imag, real], 1)], 0
        )
    high = lax.reduce_precision(real_form, 8, 7)
    return high.astype(jnp.bfloat16), (real_form - high).astype(jnp.bfloat16)


def neighbours(block, axis, width):
    count = lax.axis_size(axis)
    ahead = [(i, i + 1) for i in range(count - 1)]
    back = [(target, source) for source, target in ahead]
    return (
        lax.ppermute(block[:, -width:], axis, ahead),
        lax.ppermute(block[:, :width], axis, back),
    )


def staged_on_device(raw_first, raw_second, offsets, chirp_lengths):
    lines_count = raw_first.shape[1]
    range_count = raw_first.shape[2]
    azimuth_count = lines_count * lax.axis_size("az")
    longest = min(range_count, azimuth_count) // 4
    segments = chirp_segments(chirp_lengths[0], longest // TILE + 1)
    first_ranged = range_focus(raw_first, segments, offsets[1:2], False)
    second_ranged = range_focus(raw_second, segments, offsets[1:2], True)
    first_turned = lax.all_to_all(first_ranged, "az", split_axis=0, concat_axis=0, tiled=True)
    second_turned = lax.all_to_all(second_ranged, "az", split_axis=0, concat_axis=0, tiled=True)

    entries, left_size, right_size = tables(azimuth_count)
    left_real, left_imag, right_real, right_imag, twist_real, twist_imag = entries
    left = jnp.stack(
        stacked_tables(left_real, left_imag, True) + stacked_tables(left_real, -left_imag, True)
    )
    right = jnp.stack(
        stacked_tables(right_real, right_imag, False)
        + stacked_tables(right_real, -right_imag, False)
    )
    tabs = (left, right, jnp.stack([twist_real, twist_imag]))
    chirp_real, chirp_imag = chirp(chirp_lengths[1], azimuth_count)
    spec = forward(
        jnp.stack([chirp_real, chirp_imag]).reshape(2, 1, left_size, right_size),
        entries,
        along_forms,
    )[:, 0]
    spec = jnp.stack([spec[0], -spec[1]]) * (1.0 / azimuth_count)
    frequency = lax.broadcasted_iota(
        jnp.int32, (left_size, right_size), 0
    ) + left_size * lax.broadcasted_iota(jnp.int32, (left_size, right_size), 1)
    turns = jnp.mod(frequency * offsets[0], azimuth_count).astype(jnp.float32)
    angles = -2.0 * math.pi / azimuth_count * turns
    second_spec = complex_times(spec, jnp.cos(angles), jnp.sin(angles))

    first_image = azimuth_call(first_turned, spec, tabs)
    sums = azimuth_call(second_turned, second_spec, tabs, first_image, offsets[0:1])
    low, high = neighbours(sums, "az", 4)
    return range_box(sums, low, high)


ROWS = 8


def host_tables(lines):
    left_size, right_size = lines // LANES, LANES

    def turn(rows_count, cols_count, period):
        product = np.outer(np.arange(rows_count), np.arange(cols_count)) % period
        angles = -2.0 * np.pi / period * product
        return np.cos(angles), np.sin(angles)

    def stacked(real, imag, left):
        sign = -1.0 if left else 1.0
        form = np.block([[real, sign * imag], [-sign * imag, real]]).astype(np.float32)
        high = form.astype(jnp.bfloat16)
        low = (form - high.astype(np.float32)).astype(jnp.bfloat16)
        return [high, low]

    left_real, left_imag = turn(left_size, left_size, left_size)
    right_real, right_imag = turn(right_size, right_size, right_size)
    twist = turn(left_size, right_size, lines)
    left = np.stack(stacked(left_real, left_imag, True) + stacked(left_real, -left_imag, True))
    right = np.stack(
        stacked(right_real, right_imag, False) + stacked(right_real, -right_imag, False)
    )
    return jnp.asarray(left), jnp.asarray(right), jnp.asarray(np.stack(twist).astype(np.float32))


def chirp_values(sample, length):
    inside = (sample >= 0) & (sample < length)
    offset = 2 * jnp.clip(sample, 0, length) - length
    period = 8 * length
    square = offset * offset
    turns = jnp.floor(square.astype(jnp.float32) / period.astype(jnp.float32)).astype(jnp.int32)
    numerator = square - turns * period
    numerator = jnp.where(numerator < 0, numerator + period, numerator)
    numerator = jnp.where(numerator >= period, numerator - period, numerator)
    scale = length.astype(jnp.float32)
    angles = jnp.pi * numerator.astype(jnp.float32) / (4.0 * scale)
    amplitude = jnp.where(inside, 1.0 / jnp.sqrt(jnp.full(sample.shape, scale)), 0.0)
    return amplitude * jnp.cos(angles), amplitude * jnp.sin(angles)


def azimuth_filter(length, shift, lines, left_ref, right_ref, twist_ref, spec_ref):
    left_size = lines // LANES
    shape = (left_size, LANES)
    row, column = (lax.broadcasted_iota(jnp.int32, shape, axis) for axis in range(2))
    real, imag = chirp_values(row * LANES + column, length)
    turned = dot_split(
        (left_ref[0], left_ref[1]), split(jnp.concatenate([real, imag], axis=0))
    )
    upper, lower = turned[0:left_size], turned[left_size:]
    twist_real, twist_imag = twist_ref[0], twist_ref[1]
    stacked = jnp.concatenate(
        [upper * twist_real - lower * twist_imag, upper * twist_imag + lower * twist_real], axis=1
    )
    stacked = dot_split(split(stacked), (right_ref[0], right_ref[1])) * (1.0 / lines)
    real, imag = stacked[:, 0:LANES], -stacked[:, LANES:]
    spec_ref[0, 0], spec_ref[0, 1] = real, imag
    frequency = row + left_size * column
    turns = ((frequency * shift) & (lines - 1)).astype(jnp.float32)
    angles = (-2.0 * math.pi / lines) * turns
    turn_real, turn_imag = jnp.cos(angles), jnp.sin(angles)
    spec_ref[1, 0] = real * turn_real - imag * turn_imag
    spec_ref[1, 1] = real * turn_imag + imag * turn_real


def build_table(taps, lead, length, seg_ref, tab_ref):
    rows = seg_ref.shape[1]
    place = lax.broadcasted_iota(jnp.int32, (rows, 2 * TILE), 1)
    sample = lax.broadcasted_iota(jnp.int32, (rows, 2 * TILE), 0) * TILE - place
    sample = jnp.where(place < TILE, sample, sample + 2 * TILE) + lead
    real, imag = chirp_values(sample, length)
    seg_ref[0], seg_ref[1] = real, -imag

    def one(tap, carry):
        rows = pl.ds(pl.multiple_of(tap * TILE, TILE), TILE)
        for part in range(2):
            row = jnp.broadcast_to(seg_ref[part, pl.ds(tap, 1), :], (TILE, 2 * TILE))
            turned = pltpu.roll(row, 0, 1, stride=1, stride_axis=0)[:, 0:TILE]
            high, low = split(turned)
            columns, other = pl.ds(part * TILE, TILE), pl.ds((1 - part) * TILE, TILE)
            tab_ref[0, rows, columns] = high
            tab_ref[1, rows, columns] = low
            tab_ref[2, rows, other] = high if part == 0 else -high
            tab_ref[3, rows, other] = low if part == 0 else -low
        return carry

    lax.fori_loop(0, taps, one, 0)


def fused_kernel(
    parts, taps,
    offset_ref, length_ref, raw_first, raw_second, left_ref, right_ref, twist_ref,
    inter_out, coherence_out, windows, running,
    raw, tab, seg, spec, sent_first, sent_second, got_first, got_second, image, power,
    outer, edge_sent, edge_got,
    raw_sem, first_sem, second_send, second_recv, halo_send, halo_recv,
    edge_send_sem, edge_recv_sem,
):
    me = lax.axis_index("az")
    bins, lines_count = sent_first.shape[2], sent_first.shape[3]
    lines = parts * lines_count
    groups = bins // ROWS
    halves = lines_count // TILE
    pieces = lines_count // LANES
    blocks = WINDOW // TILE
    per_block = TILE // bins
    last = parts - 1
    middle = parts // 2
    extra = jnp.where((me == middle) | (me == middle - 1), 1, 0)

    def load(source, piece):
        width = raw.shape[2] - LANES
        rows = pl.ds(pl.multiple_of(piece * LANES, LANES), LANES)
        return pltpu.make_async_copy(
            source.at[:, rows, pl.ds(0, width)],
            raw.at[:, rows, pl.ds(LANES, width)],
            raw_sem.at[piece],
        )

    for piece in range(pieces):
        load(raw_first, piece).start()
    barrier = pltpu.get_barrier_semaphore()

    def greet(step, carry):
        pl.semaphore_signal(barrier, inc=1, device_id={"az": lax.rem(me + step, parts)})
        return carry

    lax.fori_loop(1, parts, greet, 0)
    raw[:, :, 0:LANES] = jnp.zeros((2, lines_count, LANES), jnp.bfloat16)
    build_table(taps, 0, length_ref[0], seg, tab)
    pl.semaphore_wait(barrier, parts - 1)

    half = me // (parts // 2)
    turn = lax.rem(me // per_block, blocks // 2)

    def block_of(step):
        side = lax.rem(half + 1 + step // (blocks // 2), 2)
        return side * (blocks // 2) + lax.rem(step + turn, blocks // 2)

    def correlate(block, piece, height, start, depth, target, low):
        rows = pl.ds(pl.multiple_of(piece * height, height), height)
        columns = pl.ds(pl.multiple_of(start + block * TILE, LANES), depth)
        real, imag = raw[0, rows, columns], raw[1, rows, columns]
        table = pl.ds(0, depth)
        result = (dot(real, tab[0, table]) + dot(imag, tab[2, table])) + (
            dot(real, tab[1, table]) + dot(imag, tab[3, table])
        )
        for part in range(2):
            turned = result[:, part * TILE : (part + 1) * TILE].T
            if low is not None:
                place = block * TILE + lax.broadcasted_iota(jnp.int32, (TILE, height), 0)
                turned = jnp.where(place >= low, turned, 0.0)
            turned = turned.reshape(per_block, bins, height)
            where = pl.ds(block * per_block, per_block)
            target[where, part, ROWS:bins, rows] = turned[:, 0 : bins - ROWS]
            target[where, part, 0:ROWS, rows] = turned[:, bins - ROWS : bins]

    def first_copy(piece, dest):
        rows = pl.ds(pl.multiple_of(piece * LANES, LANES), LANES)
        return pltpu.make_async_remote_copy(
            src_ref=sent_first.at[dest, :, :, rows],
            dst_ref=got_first.at[me, :, pl.ds(0, bins), rows],
            send_sem=first_sem.at[0],
            recv_sem=first_sem.at[1],
            device_id={"az": dest},
        )

    def first_whole():
        return pltpu.make_async_remote_copy(
            src_ref=sent_first.at[pl.ds(0, last)],
            dst_ref=got_first.at[pl.ds(0, last), :, pl.ds(0, bins), :],
            send_sem=first_sem.at[0],
            recv_sem=first_sem.at[1],
            device_id={"az": lax.rem(me + 1, parts)},
        )

    def first_tile(step, carry):
        block, piece = block_of(step // pieces), lax.rem(step, pieces)

        @pl.when(step < pieces)
        def _():
            load(raw_first, piece).wait()

        correlate(block, piece, LANES, LANES, taps * TILE, sent_first, None)

        def send(item, inner):
            dest = block * per_block + lax.rem(item + me, per_block)

            @pl.when(dest != me)
            def _():
                first_copy(piece, dest).start()

            return inner

        lax.fori_loop(0, per_block, send, 0)
        return carry

    lax.fori_loop(0, blocks * pieces, first_tile, 0)

    for piece in range(pieces):
        load(raw_second, piece).start()

    def halo_copy(number, side, source):
        sent, got = ((sent_first, got_first), (sent_second, got_second))[number]
        owner, start, place = ((middle, ROWS, 0), (middle - 1, ROWS // 2, ROWS // 2))[side]
        return pltpu.make_async_remote_copy(
            src_ref=sent.at[owner, :, pl.ds(start, ROWS // 2), :],
            dst_ref=got.at[source, :, pl.ds(bins + place, ROWS // 2), :],
            send_sem=halo_send.at[number, side],
            recv_sem=halo_recv.at[number, source],
            device_id={"az": middle - 1 + side},
        )

    def send_halo(number):
        sent, got = ((sent_first, got_first), (sent_second, got_second))[number]
        for side in range(2):
            @pl.when(me != middle - 1 + side)
            def _():
                halo_copy(number, side, me).start()

        half_rows = ROWS // 2

        @pl.when(me == middle - 1)
        def _():
            got[me, :, bins : bins + half_rows, :] = sent[middle, :, ROWS : ROWS + half_rows, :]

        @pl.when(me == middle)
        def _():
            got[me, :, bins + half_rows : bins + ROWS, :] = sent[middle - 1, :, half_rows:ROWS, :]

    def halo_arrived(number):
        for side in range(2):
            @pl.when(me == middle - 1 + side)
            def _():
                def one(step, carry):
                    source = lax.rem(me + step, parts)
                    halo_copy(number, side, source).wait_recv()
                    return carry

                lax.fori_loop(1, parts, one, 0)

    def halo_left(number):
        for side in range(2):
            @pl.when(me != middle - 1 + side)
            def _():
                halo_copy(number, side, me).wait_send()

    send_halo(0)
    build_table(taps + 1, offset_ref[1] - LANES, length_ref[0], seg, tab)
    for piece in range(pieces):
        load(raw_second, piece).wait()

    def second_tile(step, carry):
        correlate(
            step // halves, lax.rem(step, halves), TILE, 0, (taps + 1) * TILE, sent_second,
            offset_ref[1],
        )
        return carry

    lax.fori_loop(0, blocks * halves, second_tile, 0)

    def second_copy(group, dest):
        rows = pl.ds(pl.multiple_of(group * ROWS, ROWS), ROWS)
        return pltpu.make_async_remote_copy(
            src_ref=sent_second.at[dest, :, rows, :],
            dst_ref=got_second.at[me, :, rows, :],
            send_sem=second_send.at[group],
            recv_sem=second_recv.at[group],
            device_id={"az": dest},
        )

    def second_whole(group):
        rows = pl.ds(pl.multiple_of(group * ROWS, ROWS), ROWS)
        return pltpu.make_async_remote_copy(
            src_ref=sent_second.at[pl.ds(0, last), :, rows, :],
            dst_ref=got_second.at[pl.ds(0, last), :, rows, :],
            send_sem=second_send.at[group],
            recv_sem=second_recv.at[group],
            device_id={"az": lax.rem(me + 1, parts)},
        )

    def send_second(start, stop):
        def send(item, carry):
            group, step = start + item // last, 1 + lax.rem(item, last)
            second_copy(group, lax.rem(me + step, parts)).start()
            return carry

        lax.fori_loop(0, (stop - start) * last, send, 0)

    early = groups // 2
    send_halo(1)
    send_second(0, early)
    got_first[me, :, 0:bins, :] = sent_first[me]
    got_second[me, :, 0:bins, :] = sent_second[me]
    running[...] = jnp.zeros((4, ROWS, lines), jnp.float32)
    azimuth_filter(length_ref[1], offset_ref[0], lines, left_ref, right_ref, twist_ref, spec)

    first_whole().wait_recv()
    halo_arrived(0)

    def first_group(group, carry):
        rows = pl.ds(pl.multiple_of(group * ROWS, ROWS), ROWS)
        real, imag = azimuth_image(
            got_first.at[:, :, rows, :], spec.at[0], left_ref, right_ref, twist_ref
        )
        image[0, rows, :] = real
        image[1, rows, :] = imag
        power[rows, :] = azimuth_box(real * real + imag * imag)
        return carry

    lax.fori_loop(0, groups + extra, first_group, 0)

    def edge_copy(side, dest):
        return pltpu.make_async_remote_copy(
            src_ref=edge_sent.at[side],
            dst_ref=edge_got.at[side],
            send_sem=edge_send_sem.at[side],
            recv_sem=edge_recv_sem.at[side],
            device_id={"az": dest},
        )

    row = lax.broadcasted_iota(jnp.int32, (ROWS, lines), 0)

    def scans(values):
        before = jnp.where(row >= 1, pltpu.roll(values, 1, 0), 0.0)
        after = values
        for step in (1, 2, 4):
            before = before + jnp.where(row >= step, pltpu.roll(before, step, 0), 0.0)
            after = after + jnp.where(
                row < ROWS - step, pltpu.roll(after, ROWS - step, 0), 0.0
            )
        return before, after

    def band(group):
        return pl.ds(pl.multiple_of(group * ROWS, ROWS), ROWS)

    def finish(group):
        rows = band(group)
        inter_out[0, rows, :], inter_out[1, rows, :], coherence_out[rows, :] = results(
            [windows[part, rows, :] for part in range(4)],
            [windows[part, band(group + 1), :] for part in range(4)],
        )

    def second_group(item, carry):
        group = lax.rem(item + groups + 1, groups + 1)

        @pl.when(item >= 0)
        def _():
            second_whole(group).wait_recv()

        @pl.when(item < 0)
        def _():
            halo_arrived(1)

        rows = band(group)
        real, imag = azimuth_image(
            got_second.at[:, :, rows, :], spec.at[1], left_ref, right_ref, twist_ref
        )
        source = lax.broadcasted_iota(jnp.int32, real.shape, 1) - offset_ref[0]
        inside = (source >= 0) & (source < lines)
        real, imag = jnp.where(inside, real, 0.0), jnp.where(inside, imag, 0.0)
        first_real, first_imag = image[0, rows, :], image[1, rows, :]
        sums = (
            azimuth_box(first_real * real + first_imag * imag),
            azimuth_box(first_imag * real - first_real * imag),
            power[rows, :],
            azimuth_box(real * real + imag * imag),
        )
        for part in range(4):
            before, after = scans(sums[part])
            outer[0, part] = before
            outer[1, part] = after

        @pl.when(item < 0)
        def _():
            for part in range(4):
                low, high = 4 * part, 4 * part + 4

                @pl.when(me == middle)
                def _():
                    edge_got[0, low:high, :] = outer[1, part, 4:8, :]

                @pl.when(me != middle)
                def _():
                    edge_got[1, low:high, :] = outer[0, part, 1:5, :]

        @pl.when(item == 0)
        def _():
            for part in range(4):
                edge_sent[0, 4 * part : 4 * part + 4, :] = outer[1, part, 4:8, :]
                windows[part, bins - ROWS : bins, :] = outer[0, part]
                windows[part, bins : bins + ROWS, :] = outer[1, part]

            @pl.when((me < last) & (me != middle - 1))
            def _():
                edge_copy(0, me + 1).start()

        @pl.when(item >= 1)
        def _():
            for part in range(4):
                windows[part, band(item - 1), :] = running[part] + outer[0, part]
                running[part] = outer[1, part]

        @pl.when(item == 1)
        def _():
            for part in range(4):
                edge_sent[1, 4 * part : 4 * part + 4, :] = outer[0, part, 1:5, :]

            @pl.when((me > 0) & (me != middle))
            def _():
                edge_copy(1, me - 1).start()

            send_second(early, groups)

        @pl.when((item >= 3) & (item < groups - 1))
        def _():
            finish(item - 2)

        @pl.when(item == groups - 2)
        def _():
            @pl.when(me > 0)
            def _():
                @pl.when(me != middle)
                def _():
                    edge_copy(0, me - 1).wait_recv()

                for part in range(4):
                    windows[part, 4:8, :] += edge_got[0, 4 * part : 4 * part + 4, :]

            @pl.when(me < last)
            def _():
                @pl.when(me != middle - 1)
                def _():
                    edge_copy(1, me + 1).wait_recv()

                for part in range(4):
                    windows[part, bins + 1 : bins + 5, :] += edge_got[
                        1, 4 * part : 4 * part + 4, :
                    ]

            finish(0)

        return carry

    lax.fori_loop(0 - extra, groups, second_group, 0)
    first_whole().wait_send()

    def second_left(group, carry):
        second_whole(group).wait_send()
        return carry

    lax.fori_loop(0, groups, second_left, 0)
    halo_left(0)
    halo_left(1)

    @pl.when((me < last) & (me != middle - 1))
    def _():
        edge_copy(0, me + 1).wait_send()

    @pl.when((me > 0) & (me != middle))
    def _():
        edge_copy(1, me - 1).wait_send()


def results(now, then):
    later = lax.broadcasted_iota(jnp.int32, now[0].shape, 0) >= 5
    boxes = [pltpu.roll(jnp.where(later, now[part], then[part]), 3, 0) for part in range(4)]
    coherence = jnp.sqrt(boxes[0] * boxes[0] + boxes[1] * boxes[1]) / jnp.sqrt(
        boxes[2] * boxes[3] + 1.0
    )
    return boxes[0] * (1.0 / 64.0), boxes[1] * (1.0 / 64.0), coherence


def store_kernel(
    inter_ref, coherence_ref, windows, running, inter_out, coherence_out, inter, coherence, sems
):
    early, bins = inter_ref.shape[1], inter_out.shape[1]
    groups = (bins - early) // ROWS

    def copies(source, other, start, count, rows, number):
        return (
            pltpu.make_async_copy(
                source.at[:, pl.ds(rows, count), :],
                inter_out.at[:, pl.ds(start, count), :],
                sems.at[0, number],
            ),
            pltpu.make_async_copy(
                other.at[pl.ds(rows, count), :],
                coherence_out.at[pl.ds(start, count), :],
                sems.at[1, number],
            ),
        )

    pending = [copies(inter_ref, coherence_ref, 0, early, 0, groups)]
    for group in range(groups):
        pending.append(
            copies(inter, coherence, early + group * ROWS, ROWS, group * ROWS, group)
        )
    for copy in pending[0]:
        copy.start()
    for group in range(groups):
        now, then = (
            [windows[part, start : start + ROWS, :] for part in range(4)]
            for start in (early + group * ROWS, early + (group + 1) * ROWS)
        )
        if group == groups - 1:
            now = [now[part] + running[part] for part in range(4)]
        if group == groups - 2:
            then = [then[part] + running[part] for part in range(4)]
        rows = slice(group * ROWS, (group + 1) * ROWS)
        inter[0, rows, :], inter[1, rows, :], coherence[rows, :] = results(now, then)
        if group > 0:
            for copy in pending[group]:
                copy.start()
    for copy in pending[groups]:
        copy.start()
    for pair in pending:
        for copy in pair:
            copy.wait()


def fits(parts, lines_count, range_count):
    lines = parts * lines_count
    bins = WINDOW // parts
    return (
        lines_count % TILE == 0
        and lines & (lines - 1) == 0
        and lines // LANES == LANES // 2
        and bins % ROWS == 0
        and bins >= 6 * ROWS
        and TILE % bins == 0
        and parts % 2 == 0
        and range_count >= WINDOW + (min(range_count, lines) // 4) + 2 * TILE
    )


def on_device(raw_first, raw_second, offsets, chirp_lengths):
    parts = lax.axis_size("az")
    lines_count, range_count = raw_first.shape[1:]
    if not fits(parts, lines_count, range_count):
        return staged_on_device(raw_first, raw_second, offsets, chirp_lengths)
    lines = parts * lines_count
    bins = WINDOW // parts
    groups, early = bins // ROWS, bins - 3 * ROWS
    taps = min(range_count, lines) // 4 // TILE + 1
    depth = (taps + 1) * TILE
    left, right, twist = host_tables(lines)
    vmem = pl.BlockSpec(memory_space=pltpu.VMEM)
    smem = pl.BlockSpec(memory_space=pltpu.SMEM)
    hbm = pl.BlockSpec(memory_space=pl.ANY)
    sent = pltpu.VMEM((parts, 2, bins, lines_count), jnp.float32)
    got = pltpu.VMEM((parts, 2, bins + ROWS, lines_count), jnp.float32)
    dma = pltpu.SemaphoreType.DMA
    held = pl.pallas_call(
        functools.partial(fused_kernel, parts, taps),
        out_shape=(
            pltpu.VMEM((2, early, lines), jnp.float32),
            pltpu.VMEM((early, lines), jnp.float32),
            pltpu.VMEM((4, bins + ROWS, lines), jnp.float32),
            pltpu.VMEM((4, ROWS, lines), jnp.float32),
        ),
        in_specs=[smem, smem, hbm, hbm, vmem, vmem, vmem],
        out_specs=(vmem, vmem, vmem, vmem),
        scratch_shapes=[
            pltpu.VMEM((2, lines_count, WINDOW - TILE + depth), jnp.bfloat16),
            pltpu.VMEM((4, depth, 2 * TILE), jnp.bfloat16),
            pltpu.VMEM((2, (taps + ROWS) // ROWS * ROWS, 2 * TILE), jnp.float32),
            pltpu.VMEM((2, 2, lines // LANES, LANES), jnp.float32),
            sent,
            sent,
            got,
            got,
            pltpu.VMEM((2, bins + ROWS, lines), jnp.float32),
            pltpu.VMEM((bins + ROWS, lines), jnp.float32),
            pltpu.VMEM((2, 4, ROWS, lines), jnp.float32),
            pltpu.VMEM((2, 16, lines), jnp.float32),
            pltpu.VMEM((2, 16, lines), jnp.float32),
            dma((lines_count // LANES,)),
            dma((2,)),
            dma((groups,)),
            dma((groups,)),
            dma((2, 2)),
            dma((2, parts)),
            dma((2,)),
            dma((2,)),
        ],
        compiler_params=pltpu.CompilerParams(
            collective_id=0, has_side_effects=True, vmem_limit_bytes=49 * 1024 * 1024
        ),
        name="fused",
    )(offsets, chirp_lengths, raw_first, raw_second, left, right, twist)
    return pl.pallas_call(
        store_kernel,
        out_shape=(
            jax.ShapeDtypeStruct((2, bins, lines), jnp.float32),
            jax.ShapeDtypeStruct((bins, lines), jnp.float32),
        ),
        in_specs=[vmem, vmem, vmem, vmem],
        out_specs=(hbm, hbm),
        scratch_shapes=[
            pltpu.VMEM((2, bins - early, lines), jnp.float32),
            pltpu.VMEM((bins - early, lines), jnp.float32),
            dma((2, 4)),
        ],
        compiler_params=pltpu.CompilerParams(vmem_limit_bytes=8 * 1024 * 1024),
        name="store",
    )(*held)


def solution(mesh):
    in_specs = (P("groups", "az", None), P("groups", "az", None), P("groups"), P("groups"))
    out_specs = (P("groups", "az", None), P(("groups", "az"), None))
    return jax.shard_map(
        on_device, mesh=mesh, in_specs=in_specs, out_specs=out_specs, check_vma=False
    )
```

```python
import functools
import math

import jax
import jax.numpy as jnp
import numpy as np
from jax import lax
from jax.experimental import pallas as pl
from jax.experimental.pallas import tpu as pltpu
from jax.sharding import PartitionSpec as P

WINDOW = 1024
MAXSHIFT = 16
LANES = 128
TILE = 256
VMEM_BYTES = 60 * 1024 * 1024


along_forms = (
    ("rij", "ik", "rkj"),
    ("rkj", "jl", "rkl"),
    ("rkl", "jl", "rkj"),
    ("rkj", "ik", "rij"),
)


def padded_2(block, sides, width):
    for axis, dim in sides:
        count = lax.axis_size(axis)
        forward = [(i, i + 1) for i in range(count - 1)]
        backward = [(target, source) for source, target in forward]
        low = lax.ppermute(
            lax.slice_in_dim(block, block.shape[dim] - width, None, axis=dim), axis, forward
        )
        high = lax.ppermute(lax.slice_in_dim(block, 0, width, axis=dim), axis, backward)
        block = jnp.concatenate([low, block, high], axis=dim)
    return block


def chirp(length, samples_all):
    sample = jnp.arange(samples_all, dtype=jnp.int32)
    offset = 2 * sample - length
    period = 8 * length
    numerator = jnp.mod(offset * offset, period)
    angles = jnp.pi * numerator.astype(jnp.float32) / (4 * length).astype(jnp.float32)
    amplitude = jnp.where(sample < length, 1.0 / jnp.sqrt(length.astype(jnp.float32)), 0.0)
    return (amplitude * jnp.cos(angles), amplitude * jnp.sin(angles))


def roots(rows_count, cols_count, period):
    product = lax.broadcasted_iota(jnp.int32, (rows_count, cols_count), 0) * lax.broadcasted_iota(
        jnp.int32, (rows_count, cols_count), 1
    )
    angles = -2.0 * math.pi / period * jnp.mod(product, period).astype(jnp.float32)
    return (jnp.cos(angles), jnp.sin(angles))


def tables(length):
    right_size = LANES
    left_size = length // right_size
    entries = (
        roots(left_size, left_size, left_size)
        + roots(right_size, right_size, right_size)
        + roots(left_size, right_size, length)
    )
    return (entries, left_size, right_size)


def complex_product(form, stacked, table_real, table_imag):
    left_side, right_side, result_side = form
    matrix = jnp.stack([jnp.stack([table_real, table_imag]), jnp.stack([-table_imag, table_real])])
    return jnp.einsum(
        "c" + left_side + ",cd" + right_side + "->d" + result_side,
        stacked,
        matrix,
        precision=lax.Precision.HIGHEST,
    )


def complex_times(stacked, other_real, other_imag):
    return jnp.stack(
        [
            stacked[0] * other_real - stacked[1] * other_imag,
            stacked[0] * other_imag + stacked[1] * other_real,
        ]
    )


def forward(stacked, entries, forms):
    left_real, left_imag, right_real, right_imag, twist_real, twist_imag = entries
    stacked = complex_product(forms[0], stacked, left_real, left_imag)
    stacked = complex_times(stacked, twist_real, twist_imag)
    return complex_product(forms[1], stacked, right_real, right_imag)


def split(values):
    high = values.astype(jnp.bfloat16)
    return high, (values - high.astype(jnp.float32)).astype(jnp.bfloat16)


def dot(left, right):
    return jnp.dot(left, right, preferred_element_type=jnp.float32)


def dot_split(left, right):
    return dot(left[0], right[0]) + (dot(left[0], right[1]) + dot(left[1], right[0]))


def chirp_segments(length, taps):
    place = lax.broadcasted_iota(jnp.int32, (taps, 2 * TILE), 1)
    sample = lax.broadcasted_iota(jnp.int32, (taps, 2 * TILE), 0) * TILE - place
    sample = jnp.where(place < TILE, sample, sample + 2 * TILE)
    offset = 2 * sample - length
    numerator = jnp.mod(offset * offset, 8 * length)
    angles = jnp.pi * numerator.astype(jnp.float32) / (4 * length).astype(jnp.float32)
    inside = (sample >= 0) & (sample < length)
    amplitude = jnp.where(inside, 1.0 / jnp.sqrt(length.astype(jnp.float32)), 0.0)
    return jnp.stack([amplitude * jnp.cos(angles), -amplitude * jnp.sin(angles)], axis=1)


def range_kernel(
    taps, shifted, shift_ref, seg_ref, raw_ref, out_ref, real_high, real_low, imag_high, imag_low,
    *rest,
):
    depth = taps * TILE

    @pl.when(pl.program_id(0) == 0)
    def _():
        for tap in range(taps):
            rows = pl.ds(tap * TILE, TILE)
            turned = []
            for part in range(2):
                row = jnp.broadcast_to(seg_ref[tap, pl.ds(part, 1), :], (TILE, 2 * TILE))
                turned.append(pltpu.roll(row, 0, 1, stride=1, stride_axis=0)[:, 0:TILE])
            for part, (columns, high_ref, low_ref) in enumerate(
                (
                    (0, real_high, real_low),
                    (TILE, real_high, real_low),
                )
            ):
                high, low = split(turned[part])
                high_ref[rows, pl.ds(columns, TILE)] = high
                low_ref[rows, pl.ds(columns, TILE)] = low
                if part == 0:
                    imag_high[rows, pl.ds(TILE, TILE)] = high
                    imag_low[rows, pl.ds(TILE, TILE)] = low
                else:
                    imag_high[rows, pl.ds(0, TILE)] = -high
                    imag_low[rows, pl.ds(0, TILE)] = -low
            if shifted:
                edge_real_high, edge_real_low, edge_imag_high, edge_imag_low = rest[1:]
                real, imag = turned[0][:, 0:LANES], turned[1][:, 0:LANES]
                low_half = lax.broadcasted_iota(jnp.int32, (TILE, LANES), 1) < LANES // 2
                high, low = split(jnp.where(low_half, real, pltpu.roll(imag, LANES // 2, 1)))
                edge_real_high[rows], edge_real_low[rows] = high, low
                high, low = split(jnp.where(low_half, -imag, pltpu.roll(real, LANES // 2, 1)))
                edge_imag_high[rows], edge_imag_low[rows] = high, low

    def correlated(start, tabs):
        columns = pl.ds(start, depth)
        real, imag = raw_ref[0, :, columns], raw_ref[1, :, columns]
        return (dot(real, tabs[0][...]) + dot(imag, tabs[2][...])) + (
            dot(real, tabs[1][...]) + dot(imag, tabs[3][...])
        )

    tabs = (real_high, real_low, imag_high, imag_low)
    bins = out_ref.shape[2]
    for block in range(WINDOW // TILE):
        result = correlated(block * TILE, tabs)
        for part in range(2):
            turned = result[:, part * TILE : (part + 1) * TILE].T
            if shifted:
                rest[0][part, pl.ds(MAXSHIFT + block * TILE, TILE), :] = turned
            else:
                out_ref[pl.ds(block * TILE // bins, TILE // bins), part] = turned.reshape(
                    TILE // bins, bins, turned.shape[1]
                )
    if shifted:
        target = rest[0]
        edge = correlated(WINDOW, rest[1:]).T
        for part in range(2):
            target[part, 0:MAXSHIFT, :] = jnp.zeros((MAXSHIFT, edge.shape[1]), jnp.float32)
            target[part, pl.ds(MAXSHIFT + WINDOW, MAXSHIFT), :] = edge[
                part * LANES // 2 : part * LANES // 2 + MAXSHIFT
            ]
        held = WINDOW + 2 * MAXSHIFT
        turn = lax.rem(held - MAXSHIFT + shift_ref[0], held)
        for part in range(2):
            moved = pltpu.roll(target[part], turn, 0)[0:WINDOW]
            out_ref[:, part] = moved.reshape(WINDOW // bins, bins, moved.shape[1])


def range_focus(raw, segments, shift, shifted):
    parts = lax.axis_size("az")
    bins = WINDOW // parts
    taps = segments.shape[0]
    depth = taps * TILE
    lines_count = raw.shape[1]
    height = min(TILE, lines_count)
    width = depth + WINDOW
    scratch = [pltpu.VMEM((depth, 2 * TILE), jnp.bfloat16)] * 4
    if shifted:
        scratch += [pltpu.VMEM((2, WINDOW + 2 * MAXSHIFT, height), jnp.float32)]
        scratch += [pltpu.VMEM((depth, LANES), jnp.bfloat16)] * 4
    return pl.pallas_call(
        functools.partial(range_kernel, taps, shifted),
        out_shape=jax.ShapeDtypeStruct((parts, 2, bins, lines_count), jnp.float32),
        grid=(lines_count // height,),
        in_specs=[
            pl.BlockSpec(memory_space=pltpu.SMEM),
            pl.BlockSpec((taps, 2, 2 * TILE), lambda i: (0, 0, 0)),
            pl.BlockSpec((2, height, width), lambda i: (0, i, 0)),
        ],
        out_specs=pl.BlockSpec((parts, 2, bins, height), lambda i: (0, 0, 0, i)),
        scratch_shapes=scratch,
        compiler_params=pltpu.CompilerParams(vmem_limit_bytes=VMEM_BYTES),
        cost_estimate=pl.CostEstimate(
            flops=16 * lines_count * depth * WINDOW,
            bytes_accessed=4 * lines_count * (width + 2 * WINDOW),
            transcendentals=0,
        ),
        name="range_second" if shifted else "range_first",
    )(shift, segments, raw)


def azimuth_image(in_ref, spec_ref, left_ref, right_ref, twist_ref):
    parts, _, bins, lines_count = in_ref.shape
    lines = parts * lines_count
    left_size = lines // LANES
    real, imag = (
        jnp.concatenate([in_ref[one, part] for one in range(parts)], axis=1).reshape(
            bins, left_size, LANES
        )
        for part in range(2)
    )
    twist_real, twist_imag = twist_ref[0], twist_ref[1]
    middle_real, middle_imag = [], []
    for one in range(0, bins, 2):
        pair = jnp.concatenate(
            [
                jnp.concatenate([real[one], imag[one]], axis=0),
                jnp.concatenate([real[one + 1], imag[one + 1]], axis=0),
            ],
            axis=1,
        )
        turned = dot_split((left_ref[0], left_ref[1]), split(pair))
        for half in range(2):
            columns = slice(half * LANES, (half + 1) * LANES)
            upper, lower = turned[0:left_size, columns], turned[left_size:, columns]
            middle_real.append(upper * twist_real - lower * twist_imag)
            middle_imag.append(upper * twist_imag + lower * twist_real)
    stacked = jnp.concatenate(
        [jnp.concatenate(middle_real, axis=0), jnp.concatenate(middle_imag, axis=0)], axis=1
    )
    spectrum = dot_split(split(stacked), (right_ref[0], right_ref[1]))
    upper = spectrum[:, 0:LANES].reshape(bins, left_size, LANES)
    lower = spectrum[:, LANES:].reshape(bins, left_size, LANES)
    spec_real, spec_imag = spec_ref[0][None], spec_ref[1][None]
    stacked = jnp.concatenate(
        [
            (upper * spec_real - lower * spec_imag).reshape(bins * left_size, LANES),
            (upper * spec_imag + lower * spec_real).reshape(bins * left_size, LANES),
        ],
        axis=1,
    )
    stacked = dot_split(split(stacked), (right_ref[2], right_ref[3]))
    upper = stacked[:, 0:LANES].reshape(bins, left_size, LANES)
    lower = stacked[:, LANES:].reshape(bins, left_size, LANES)
    middle_real = upper * twist_real[None] + lower * twist_imag[None]
    middle_imag = lower * twist_real[None] - upper * twist_imag[None]
    result_real, result_imag = [], []
    for one in range(0, bins, 2):
        pair = jnp.concatenate(
            [
                jnp.concatenate([middle_real[one], middle_imag[one]], axis=0),
                jnp.concatenate([middle_real[one + 1], middle_imag[one + 1]], axis=0),
            ],
            axis=1,
        )
        turned = dot_split((left_ref[2], left_ref[3]), split(pair))
        for half in range(2):
            columns = slice(half * LANES, (half + 1) * LANES)
            result_real.append(turned[0:left_size, columns])
            result_imag.append(turned[left_size:, columns])
    return (
        jnp.stack(result_real).reshape(bins, lines),
        jnp.stack(result_imag).reshape(bins, lines),
    )


def first_kernel(in_ref, spec_ref, left_ref, right_ref, twist_ref, out_ref):
    out_ref[0], out_ref[1] = azimuth_image(in_ref, spec_ref, left_ref, right_ref, twist_ref)


def azimuth_box(values):
    rows, lines = values.shape
    values = jnp.concatenate([values, jnp.zeros((rows, LANES), jnp.float32)], axis=1)
    total = lines + LANES
    for step in (1, 2, 4):
        values = values + pltpu.roll(values, total - step, 1)
    return pltpu.roll(values, 3, 1)[:, 0:lines]


def second_kernel(
    shift_ref, in_ref, first_ref, spec_ref, left_ref, right_ref, twist_ref, out_ref
):
    real, imag = azimuth_image(in_ref, spec_ref, left_ref, right_ref, twist_ref)
    source = lax.broadcasted_iota(jnp.int32, real.shape, 1) - shift_ref[0]
    inside = (source >= 0) & (source < real.shape[1])
    real, imag = jnp.where(inside, real, 0.0), jnp.where(inside, imag, 0.0)
    first_real, first_imag = first_ref[0], first_ref[1]
    out_ref[0] = azimuth_box(first_real * real + first_imag * imag)
    out_ref[1] = azimuth_box(first_imag * real - first_real * imag)
    out_ref[2] = azimuth_box(first_real * first_real + first_imag * first_imag)
    out_ref[3] = azimuth_box(real * real + imag * imag)


def azimuth_call(ranged, spec, tabs, first=None, shift=None):
    left, right, twist = tabs
    parts, _, bins, lines_count = ranged.shape
    lines = parts * lines_count
    height = 8

    def whole(array):
        return pl.BlockSpec(array.shape, lambda i: (0,) * array.ndim)

    block = pl.BlockSpec((2, height, lines), lambda i: (0, i, 0))
    source = pl.BlockSpec((parts, 2, height, lines_count), lambda i: (0, 0, i, 0))
    operands, specs = [ranged], [source]
    if first is not None:
        operands = [shift, ranged, first]
        specs = [pl.BlockSpec(memory_space=pltpu.SMEM), source, block]
    constants = [spec, left, right, twist]
    outs = 2 if first is None else 4
    return pl.pallas_call(
        first_kernel if first is None else second_kernel,
        out_shape=jax.ShapeDtypeStruct((outs, bins, lines), jnp.float32),
        grid=(bins // height,),
        in_specs=specs + [whole(array) for array in constants],
        out_specs=pl.BlockSpec((outs, height, lines), lambda i: (0, i, 0)),
        compiler_params=pltpu.CompilerParams(vmem_limit_bytes=VMEM_BYTES),
        cost_estimate=pl.CostEstimate(
            flops=24 * 512 * bins * lines,
            bytes_accessed=4 * bins * lines * (2 + outs),
            transcendentals=0,
        ),
        name="azimuth_first" if first is None else "azimuth_second",
    )(*operands, *constants)


def range_box_kernel(sums_ref, low_ref, high_ref, inter_ref, coherence_ref, scratch):
    bins = sums_ref.shape[1]
    boxes = []
    for part in range(4):
        scratch[4:8, :] = low_ref[part]
        scratch[pl.ds(8, bins), :] = sums_ref[part]
        scratch[pl.ds(8 + bins, 4), :] = high_ref[part]
        values = scratch[pl.ds(5, bins + 7), :]
        values = values[:-1] + values[1:]
        values = values[:-2] + values[2:]
        boxes.append(values[:-4] + values[4:])
    inter_ref[0] = boxes[0] * (1.0 / 64.0)
    inter_ref[1] = boxes[1] * (1.0 / 64.0)
    coherence_ref[...] = jnp.sqrt(boxes[0] * boxes[0] + boxes[1] * boxes[1]) / jnp.sqrt(
        boxes[2] * boxes[3] + 1.0
    )


def range_box(sums, low, high):
    _, bins, lines = sums.shape
    width = 512
    return pl.pallas_call(
        range_box_kernel,
        out_shape=(
            jax.ShapeDtypeStruct((2, bins, lines), jnp.float32),
            jax.ShapeDtypeStruct((bins, lines), jnp.float32),
        ),
        grid=(lines // width,),
        in_specs=[
            pl.BlockSpec((4, bins, width), lambda i: (0, 0, i)),
            pl.BlockSpec((4, 4, width), lambda i: (0, 0, i)),
            pl.BlockSpec((4, 4, width), lambda i: (0, 0, i)),
        ],
        out_specs=(
            pl.BlockSpec((2, bins, width), lambda i: (0, 0, i)),
            pl.BlockSpec((bins, width), lambda i: (0, i)),
        ),
        scratch_shapes=[pltpu.VMEM((bins + 16, width), jnp.float32)],
        compiler_params=pltpu.CompilerParams(vmem_limit_bytes=VMEM_BYTES),
        name="range_box",
    )(sums, low, high)


def stacked_tables(real, imag, left):
    if left:
        real_form = jnp.concatenate(
            [jnp.concatenate([real, -imag], 1), jnp.concatenate([imag, real], 1)], 0
        )
    else:
        real_form = jnp.concatenate(
            [jnp.concatenate([real, imag], 1), jnp.concatenate([-imag, real], 1)], 0
        )
    high = lax.reduce_precision(real_form, 8, 7)
    return high.astype(jnp.bfloat16), (real_form - high).astype(jnp.bfloat16)


def neighbours(block, axis, width):
    count = lax.axis_size(axis)
    ahead = [(i, i + 1) for i in range(count - 1)]
    back = [(target, source) for source, target in ahead]
    return (
        lax.ppermute(block[:, -width:], axis, ahead),
        lax.ppermute(block[:, :width], axis, back),
    )


def staged_on_device(raw_first, raw_second, offsets, chirp_lengths):
    lines_count = raw_first.shape[1]
    range_count = raw_first.shape[2]
    azimuth_count = lines_count * lax.axis_size("az")
    longest = min(range_count, azimuth_count) // 4
    segments = chirp_segments(chirp_lengths[0], longest // TILE + 1)
    first_ranged = range_focus(raw_first, segments, offsets[1:2], False)
    second_ranged = range_focus(raw_second, segments, offsets[1:2], True)
    first_turned = lax.all_to_all(first_ranged, "az", split_axis=0, concat_axis=0, tiled=True)
    second_turned = lax.all_to_all(second_ranged, "az", split_axis=0, concat_axis=0, tiled=True)

    entries, left_size, right_size = tables(azimuth_count)
    left_real, left_imag, right_real, right_imag, twist_real, twist_imag = entries
    left = jnp.stack(
        stacked_tables(left_real, left_imag, True) + stacked_tables(left_real, -left_imag, True)
    )
    right = jnp.stack(
        stacked_tables(right_real, right_imag, False)
        + stacked_tables(right_real, -right_imag, False)
    )
    tabs = (left, right, jnp.stack([twist_real, twist_imag]))
    chirp_real, chirp_imag = chirp(chirp_lengths[1], azimuth_count)
    spec = forward(
        jnp.stack([chirp_real, chirp_imag]).reshape(2, 1, left_size, right_size),
        entries,
        along_forms,
    )[:, 0]
    spec = jnp.stack([spec[0], -spec[1]]) * (1.0 / azimuth_count)
    frequency = lax.broadcasted_iota(
        jnp.int32, (left_size, right_size), 0
    ) + left_size * lax.broadcasted_iota(jnp.int32, (left_size, right_size), 1)
    turns = jnp.mod(frequency * offsets[0], azimuth_count).astype(jnp.float32)
    angles = -2.0 * math.pi / azimuth_count * turns
    second_spec = complex_times(spec, jnp.cos(angles), jnp.sin(angles))

    first_image = azimuth_call(first_turned, spec, tabs)
    sums = azimuth_call(second_turned, second_spec, tabs, first_image, offsets[0:1])
    low, high = neighbours(sums, "az", 4)
    return range_box(sums, low, high)


ROWS = 8


def host_tables(lines):
    left_size, right_size = lines // LANES, LANES

    def turn(rows_count, cols_count, period):
        product = np.outer(np.arange(rows_count), np.arange(cols_count)) % period
        angles = -2.0 * np.pi / period * product
        return np.cos(angles), np.sin(angles)

    def stacked(real, imag, left):
        sign = -1.0 if left else 1.0
        form = np.block([[real, sign * imag], [-sign * imag, real]]).astype(np.float32)
        high = form.astype(jnp.bfloat16)
        low = (form - high.astype(np.float32)).astype(jnp.bfloat16)
        return [high, low]

    left_real, left_imag = turn(left_size, left_size, left_size)
    right_real, right_imag = turn(right_size, right_size, right_size)
    twist = turn(left_size, right_size, lines)
    left = np.stack(stacked(left_real, left_imag, True) + stacked(left_real, -left_imag, True))
    right = np.stack(
        stacked(right_real, right_imag, False) + stacked(right_real, -right_imag, False)
    )
    return jnp.asarray(left), jnp.asarray(right), jnp.asarray(np.stack(twist).astype(np.float32))


def chirp_values(sample, length):
    inside = (sample >= 0) & (sample < length)
    offset = 2 * jnp.clip(sample, 0, length) - length
    period = 8 * length
    square = offset * offset
    turns = jnp.floor(square.astype(jnp.float32) / period.astype(jnp.float32)).astype(jnp.int32)
    numerator = square - turns * period
    numerator = jnp.where(numerator < 0, numerator + period, numerator)
    numerator = jnp.where(numerator >= period, numerator - period, numerator)
    scale = length.astype(jnp.float32)
    angles = jnp.pi * numerator.astype(jnp.float32) / (4.0 * scale)
    amplitude = jnp.where(inside, 1.0 / jnp.sqrt(jnp.full(sample.shape, scale)), 0.0)
    return amplitude * jnp.cos(angles), amplitude * jnp.sin(angles)


def azimuth_filter(length, shift, lines, left_ref, right_ref, twist_ref, spec_ref):
    left_size = lines // LANES
    shape = (left_size, LANES)
    row, column = (lax.broadcasted_iota(jnp.int32, shape, axis) for axis in range(2))
    real, imag = chirp_values(row * LANES + column, length)
    turned = dot_split(
        (left_ref[0], left_ref[1]), split(jnp.concatenate([real, imag], axis=0))
    )
    upper, lower = turned[0:left_size], turned[left_size:]
    twist_real, twist_imag = twist_ref[0], twist_ref[1]
    stacked = jnp.concatenate(
        [upper * twist_real - lower * twist_imag, upper * twist_imag + lower * twist_real], axis=1
    )
    stacked = dot_split(split(stacked), (right_ref[0], right_ref[1])) * (1.0 / lines)
    real, imag = stacked[:, 0:LANES], -stacked[:, LANES:]
    spec_ref[0, 0], spec_ref[0, 1] = real, imag
    frequency = row + left_size * column
    turns = ((frequency * shift) & (lines - 1)).astype(jnp.float32)
    angles = (-2.0 * math.pi / lines) * turns
    turn_real, turn_imag = jnp.cos(angles), jnp.sin(angles)
    spec_ref[1, 0] = real * turn_real - imag * turn_imag
    spec_ref[1, 1] = real * turn_imag + imag * turn_real


def build_table(taps, lead, length, seg_ref, tab_ref):
    rows = seg_ref.shape[1]
    place = lax.broadcasted_iota(jnp.int32, (rows, 2 * TILE), 1)
    sample = lax.broadcasted_iota(jnp.int32, (rows, 2 * TILE), 0) * TILE - place
    sample = jnp.where(place < TILE, sample, sample + 2 * TILE) + lead
    real, imag = chirp_values(sample, length)
    seg_ref[0], seg_ref[1] = real, -imag

    def one(tap, carry):
        rows = pl.ds(pl.multiple_of(tap * TILE, TILE), TILE)
        for part in range(2):
            row = jnp.broadcast_to(seg_ref[part, pl.ds(tap, 1), :], (TILE, 2 * TILE))
            turned = pltpu.roll(row, 0, 1, stride=1, stride_axis=0)[:, 0:TILE]
            high, low = split(turned)
            columns, other = pl.ds(part * TILE, TILE), pl.ds((1 - part) * TILE, TILE)
            tab_ref[0, rows, columns] = high
            tab_ref[1, rows, columns] = low
            tab_ref[2, rows, other] = high if part == 0 else -high
            tab_ref[3, rows, other] = low if part == 0 else -low
        return carry

    lax.fori_loop(0, taps, one, 0)


def fused_kernel(
    parts, taps,
    offset_ref, length_ref, raw_first, raw_second, left_ref, right_ref, twist_ref,
    inter_out, coherence_out, windows, running,
    raw, tab, seg, spec, sent_first, sent_second, got_first, got_second, image, power,
    outer, edge_sent, edge_got,
    raw_sem, first_sem, second_send, second_recv, halo_send, halo_recv,
    edge_send_sem, edge_recv_sem,
):
    me = lax.axis_index("az")
    bins, lines_count = sent_first.shape[2], sent_first.shape[3]
    lines = parts * lines_count
    groups = bins // ROWS
    halves = lines_count // TILE
    pieces = lines_count // LANES
    blocks = WINDOW // TILE
    per_block = TILE // bins
    last = parts - 1
    middle = parts // 2
    extra = jnp.where((me == middle) | (me == middle - 1), 1, 0)

    def load(source, piece):
        width = raw.shape[2] - LANES
        rows = pl.ds(pl.multiple_of(piece * LANES, LANES), LANES)
        return pltpu.make_async_copy(
            source.at[:, rows, pl.ds(0, width)],
            raw.at[:, rows, pl.ds(LANES, width)],
            raw_sem.at[piece],
        )

    for piece in range(pieces):
        load(raw_first, piece).start()
    barrier = pltpu.get_barrier_semaphore()

    def greet(step, carry):
        pl.semaphore_signal(barrier, inc=1, device_id={"az": lax.rem(me + step, parts)})
        return carry

    lax.fori_loop(1, parts, greet, 0)
    raw[:, :, 0:LANES] = jnp.zeros((2, lines_count, LANES), jnp.bfloat16)
    build_table(taps, 0, length_ref[0], seg, tab)

    half = me // (parts // 2)
    turn = lax.rem(me // per_block, blocks // 2)

    def block_of(step):
        side = lax.rem(half + 1 + step // (blocks // 2), 2)
        return side * (blocks // 2) + lax.rem(step + turn, blocks // 2)

    def correlate(block, piece, height, start, depth, target, low):
        rows = pl.ds(pl.multiple_of(piece * height, height), height)
        columns = pl.ds(pl.multiple_of(start + block * TILE, LANES), depth)
        real, imag = raw[0, rows, columns], raw[1, rows, columns]
        table = pl.ds(0, depth)
        result = (dot(real, tab[0, table]) + dot(imag, tab[2, table])) + (
            dot(real, tab[1, table]) + dot(imag, tab[3, table])
        )
        for part in range(2):
            turned = result[:, part * TILE : (part + 1) * TILE].T
            if low is not None:
                place = block * TILE + lax.broadcasted_iota(jnp.int32, (TILE, height), 0)
                turned = jnp.where(place >= low, turned, 0.0)
            turned = turned.reshape(per_block, bins, height)
            where = pl.ds(block * per_block, per_block)
            target[where, part, ROWS:bins, rows] = turned[:, 0 : bins - ROWS]
            target[where, part, 0:ROWS, rows] = turned[:, bins - ROWS : bins]

    def first_copy(piece, dest):
        rows = pl.ds(pl.multiple_of(piece * LANES, LANES), LANES)
        return pltpu.make_async_remote_copy(
            src_ref=sent_first.at[dest, :, :, rows],
            dst_ref=got_first.at[me, :, pl.ds(0, bins), rows],
            send_sem=first_sem.at[0],
            recv_sem=first_sem.at[1],
            device_id={"az": dest},
        )

    def first_whole():
        return pltpu.make_async_remote_copy(
            src_ref=sent_first.at[pl.ds(0, last)],
            dst_ref=got_first.at[pl.ds(0, last), :, pl.ds(0, bins), :],
            send_sem=first_sem.at[0],
            recv_sem=first_sem.at[1],
            device_id={"az": lax.rem(me + 1, parts)},
        )

    def first_tile(step, carry):
        block, piece = block_of(step // pieces), lax.rem(step, pieces)

        @pl.when(step < pieces)
        def _():
            load(raw_first, piece).wait()

        correlate(block, piece, LANES, LANES, taps * TILE, sent_first, None)

        @pl.when(step == 0)
        def _():
            pl.semaphore_wait(barrier, parts - 1)

        def send(item, inner):
            dest = block * per_block + lax.rem(item + me, per_block)

            @pl.when(dest != me)
            def _():
                first_copy(piece, dest).start()

            return inner

        lax.fori_loop(0, per_block, send, 0)
        return carry

    lax.fori_loop(0, blocks * pieces, first_tile, 0)

    for piece in range(pieces):
        load(raw_second, piece).start()

    def halo_copy(number, side, source):
        sent, got = ((sent_first, got_first), (sent_second, got_second))[number]
        owner, start, place, count = ((middle, ROWS, 0, 4), (middle - 1, 5, 5, 3))[side]
        return pltpu.make_async_remote_copy(
            src_ref=sent.at[owner, :, pl.ds(start, count), :],
            dst_ref=got.at[source, :, pl.ds(bins + place, count), :],
            send_sem=halo_send.at[number, side],
            recv_sem=halo_recv.at[number, source],
            device_id={"az": middle - 1 + side},
        )

    def send_halo(number):
        sent, got = ((sent_first, got_first), (sent_second, got_second))[number]
        for side in range(2):
            @pl.when(me != middle - 1 + side)
            def _():
                halo_copy(number, side, me).start()

        @pl.when(me == middle - 1)
        def _():
            got[me, :, bins : bins + 4, :] = sent[middle, :, ROWS : ROWS + 4, :]

        @pl.when(me == middle)
        def _():
            got[me, :, bins + 5 : bins + ROWS, :] = sent[middle - 1, :, 5:ROWS, :]

    def halo_arrived(number):
        for side in range(2):
            @pl.when(me == middle - 1 + side)
            def _():
                def one(step, carry):
                    source = lax.rem(me + step, parts)
                    halo_copy(number, side, source).wait_recv()
                    return carry

                lax.fori_loop(1, parts, one, 0)

    def halo_left(number):
        for side in range(2):
            @pl.when(me != middle - 1 + side)
            def _():
                halo_copy(number, side, me).wait_send()

    send_halo(0)
    build_table(taps + 1, offset_ref[1] - LANES, length_ref[0], seg, tab)
    for piece in range(pieces):
        load(raw_second, piece).wait()

    def second_tile(step, carry):
        correlate(
            step // halves, lax.rem(step, halves), TILE, 0, (taps + 1) * TILE, sent_second,
            offset_ref[1],
        )
        return carry

    lax.fori_loop(0, blocks * halves, second_tile, 0)

    def second_copy(group, dest):
        rows = pl.ds(pl.multiple_of(group * ROWS, ROWS), ROWS)
        return pltpu.make_async_remote_copy(
            src_ref=sent_second.at[dest, :, rows, :],
            dst_ref=got_second.at[me, :, rows, :],
            send_sem=second_send.at[group],
            recv_sem=second_recv.at[group],
            device_id={"az": dest},
        )

    def second_whole(group):
        rows = pl.ds(pl.multiple_of(group * ROWS, ROWS), ROWS)
        return pltpu.make_async_remote_copy(
            src_ref=sent_second.at[pl.ds(0, last), :, rows, :],
            dst_ref=got_second.at[pl.ds(0, last), :, rows, :],
            send_sem=second_send.at[group],
            recv_sem=second_recv.at[group],
            device_id={"az": lax.rem(me + 1, parts)},
        )

    def send_second(start, stop):
        def send(item, carry):
            group, step = start + item // last, 1 + lax.rem(item, last)
            second_copy(group, lax.rem(me + step, parts)).start()
            return carry

        lax.fori_loop(0, (stop - start) * last, send, 0)

    early = groups // 2
    send_halo(1)
    send_second(0, early)
    got_first[me, :, 0:bins, :] = sent_first[me]
    got_second[me, :, 0:bins, :] = sent_second[me]
    running[...] = jnp.zeros((4, ROWS, lines), jnp.float32)
    azimuth_filter(length_ref[1], offset_ref[0], lines, left_ref, right_ref, twist_ref, spec)

    first_whole().wait_recv()
    halo_arrived(0)

    def first_group(group, carry):
        rows = pl.ds(pl.multiple_of(group * ROWS, ROWS), ROWS)
        real, imag = azimuth_image(
            got_first.at[:, :, rows, :], spec.at[0], left_ref, right_ref, twist_ref
        )
        image[0, rows, :] = real
        image[1, rows, :] = imag
        power[rows, :] = azimuth_box(real * real + imag * imag)
        return carry

    lax.fori_loop(0, groups + extra, first_group, 0)

    def edge_copy(side, dest):
        return pltpu.make_async_remote_copy(
            src_ref=edge_sent.at[side],
            dst_ref=edge_got.at[side],
            send_sem=edge_send_sem.at[side],
            recv_sem=edge_recv_sem.at[side],
            device_id={"az": dest},
        )

    row = lax.broadcasted_iota(jnp.int32, (ROWS, lines), 0)

    def scans(values):
        before = jnp.where(row >= 1, pltpu.roll(values, 1, 0), 0.0)
        after = values
        for step in (1, 2, 4):
            before = before + jnp.where(row >= step, pltpu.roll(before, step, 0), 0.0)
            after = after + jnp.where(
                row < ROWS - step, pltpu.roll(after, ROWS - step, 0), 0.0
            )
        return before, after

    def band(group):
        return pl.ds(pl.multiple_of(group * ROWS, ROWS), ROWS)

    def finish(group):
        rows = band(group)
        inter_out[0, rows, :], inter_out[1, rows, :], coherence_out[rows, :] = results(
            [windows[part, rows, :] for part in range(4)],
            [windows[part, band(group + 1), :] for part in range(4)],
        )

    def second_group(item, carry):
        group = lax.rem(item + groups + 1, groups + 1)

        @pl.when(item >= 0)
        def _():
            second_whole(group).wait_recv()

        @pl.when(item < 0)
        def _():
            halo_arrived(1)

        rows = band(group)
        real, imag = azimuth_image(
            got_second.at[:, :, rows, :], spec.at[1], left_ref, right_ref, twist_ref
        )
        source = lax.broadcasted_iota(jnp.int32, real.shape, 1) - offset_ref[0]
        inside = (source >= 0) & (source < lines)
        real, imag = jnp.where(inside, real, 0.0), jnp.where(inside, imag, 0.0)
        first_real, first_imag = image[0, rows, :], image[1, rows, :]
        sums = (
            azimuth_box(first_real * real + first_imag * imag),
            azimuth_box(first_imag * real - first_real * imag),
            power[rows, :],
            azimuth_box(real * real + imag * imag),
        )
        for part in range(4):
            before, after = scans(sums[part])
            outer[0, part] = before
            outer[1, part] = after

        @pl.when(item < 0)
        def _():
            for part in range(4):
                low, high = 4 * part, 4 * part + 4

                @pl.when(me == middle)
                def _():
                    edge_got[0, low:high, :] = outer[1, part, 4:8, :]

                @pl.when(me != middle)
                def _():
                    edge_got[1, low:high, :] = outer[0, part, 1:5, :]

        @pl.when(item == 0)
        def _():
            for part in range(4):
                edge_sent[0, 4 * part : 4 * part + 4, :] = outer[1, part, 4:8, :]
                windows[part, bins - ROWS : bins, :] = outer[0, part]
                windows[part, bins : bins + ROWS, :] = outer[1, part]

            @pl.when((me < last) & (me != middle - 1))
            def _():
                edge_copy(0, me + 1).start()

        @pl.when(item >= 1)
        def _():
            for part in range(4):
                windows[part, band(item - 1), :] = running[part] + outer[0, part]
                running[part] = outer[1, part]

        @pl.when(item == 1)
        def _():
            for part in range(4):
                edge_sent[1, 4 * part : 4 * part + 4, :] = outer[0, part, 1:5, :]

            @pl.when((me > 0) & (me != middle))
            def _():
                edge_copy(1, me - 1).start()

            send_second(early, groups)

        @pl.when((item >= 3) & (item < groups - 1))
        def _():
            finish(item - 2)

        @pl.when(item == groups - 2)
        def _():
            @pl.when(me > 0)
            def _():
                @pl.when(me != middle)
                def _():
                    edge_copy(0, me - 1).wait_recv()

                for part in range(4):
                    windows[part, 4:8, :] += edge_got[0, 4 * part : 4 * part + 4, :]

            @pl.when(me < last)
            def _():
                @pl.when(me != middle - 1)
                def _():
                    edge_copy(1, me + 1).wait_recv()

                for part in range(4):
                    windows[part, bins + 1 : bins + 5, :] += edge_got[
                        1, 4 * part : 4 * part + 4, :
                    ]

            finish(0)

        return carry

    lax.fori_loop(0 - extra, groups, second_group, 0)
    first_whole().wait_send()

    def second_left(group, carry):
        second_whole(group).wait_send()
        return carry

    lax.fori_loop(0, groups, second_left, 0)
    halo_left(0)
    halo_left(1)

    @pl.when((me < last) & (me != middle - 1))
    def _():
        edge_copy(0, me + 1).wait_send()

    @pl.when((me > 0) & (me != middle))
    def _():
        edge_copy(1, me - 1).wait_send()


def results(now, then):
    later = lax.broadcasted_iota(jnp.int32, now[0].shape, 0) >= 5
    boxes = [pltpu.roll(jnp.where(later, now[part], then[part]), 3, 0) for part in range(4)]
    coherence = jnp.sqrt(boxes[0] * boxes[0] + boxes[1] * boxes[1]) / jnp.sqrt(
        boxes[2] * boxes[3] + 1.0
    )
    return boxes[0] * (1.0 / 64.0), boxes[1] * (1.0 / 64.0), coherence


def store_kernel(
    inter_ref, coherence_ref, windows, running, inter_out, coherence_out, inter, coherence, sems
):
    early, bins = inter_ref.shape[1], inter_out.shape[1]
    groups = (bins - early) // ROWS

    def copies(source, other, start, count, rows, number):
        return (
            pltpu.make_async_copy(
                source.at[:, pl.ds(rows, count), :],
                inter_out.at[:, pl.ds(start, count), :],
                sems.at[0, number],
            ),
            pltpu.make_async_copy(
                other.at[pl.ds(rows, count), :],
                coherence_out.at[pl.ds(start, count), :],
                sems.at[1, number],
            ),
        )

    pending = [copies(inter_ref, coherence_ref, 0, early, 0, groups)]
    for group in range(groups):
        pending.append(
            copies(inter, coherence, early + group * ROWS, ROWS, group * ROWS, group)
        )
    for copy in pending[0]:
        copy.start()
    for group in range(groups):
        now, then = (
            [windows[part, start : start + ROWS, :] for part in range(4)]
            for start in (early + group * ROWS, early + (group + 1) * ROWS)
        )
        if group == groups - 1:
            now = [now[part] + running[part] for part in range(4)]
        if group == groups - 2:
            then = [then[part] + running[part] for part in range(4)]
        rows = slice(group * ROWS, (group + 1) * ROWS)
        inter[0, rows, :], inter[1, rows, :], coherence[rows, :] = results(now, then)
        if group > 0:
            for copy in pending[group]:
                copy.start()
    for copy in pending[groups]:
        copy.start()
    for pair in pending:
        for copy in pair:
            copy.wait()


def fits(parts, lines_count, range_count):
    lines = parts * lines_count
    bins = WINDOW // parts
    return (
        lines_count % TILE == 0
        and lines & (lines - 1) == 0
        and lines // LANES == LANES // 2
        and bins % ROWS == 0
        and bins >= 6 * ROWS
        and TILE % bins == 0
        and parts % 2 == 0
        and range_count >= WINDOW + (min(range_count, lines) // 4) + 2 * TILE
    )


def on_device(raw_first, raw_second, offsets, chirp_lengths):
    parts = lax.axis_size("az")
    lines_count, range_count = raw_first.shape[1:]
    if not fits(parts, lines_count, range_count):
        return staged_on_device(raw_first, raw_second, offsets, chirp_lengths)
    lines = parts * lines_count
    bins = WINDOW // parts
    groups, early = bins // ROWS, bins - 3 * ROWS
    taps = min(range_count, lines) // 4 // TILE + 1
    depth = (taps + 1) * TILE
    left, right, twist = host_tables(lines)
    vmem = pl.BlockSpec(memory_space=pltpu.VMEM)
    smem = pl.BlockSpec(memory_space=pltpu.SMEM)
    hbm = pl.BlockSpec(memory_space=pl.ANY)
    sent = pltpu.VMEM((parts, 2, bins, lines_count), jnp.float32)
    got = pltpu.VMEM((parts, 2, bins + ROWS, lines_count), jnp.float32)
    dma = pltpu.SemaphoreType.DMA
    held = pl.pallas_call(
        functools.partial(fused_kernel, parts, taps),
        out_shape=(
            pltpu.VMEM((2, early, lines), jnp.float32),
            pltpu.VMEM((early, lines), jnp.float32),
            pltpu.VMEM((4, bins + ROWS, lines), jnp.float32),
            pltpu.VMEM((4, ROWS, lines), jnp.float32),
        ),
        in_specs=[smem, smem, hbm, hbm, vmem, vmem, vmem],
        out_specs=(vmem, vmem, vmem, vmem),
        scratch_shapes=[
            pltpu.VMEM((2, lines_count, WINDOW - TILE + depth), jnp.bfloat16),
            pltpu.VMEM((4, depth, 2 * TILE), jnp.bfloat16),
            pltpu.VMEM((2, (taps + ROWS) // ROWS * ROWS, 2 * TILE), jnp.float32),
            pltpu.VMEM((2, 2, lines // LANES, LANES), jnp.float32),
            sent,
            sent,
            got,
            got,
            pltpu.VMEM((2, bins + ROWS, lines), jnp.float32),
            pltpu.VMEM((bins + ROWS, lines), jnp.float32),
            pltpu.VMEM((2, 4, ROWS, lines), jnp.float32),
            pltpu.VMEM((2, 16, lines), jnp.float32),
            pltpu.VMEM((2, 16, lines), jnp.float32),
            dma((lines_count // LANES,)),
            dma((2,)),
            dma((groups,)),
            dma((groups,)),
            dma((2, 2)),
            dma((2, parts)),
            dma((2,)),
            dma((2,)),
        ],
        compiler_params=pltpu.CompilerParams(
            collective_id=0, has_side_effects=True, vmem_limit_bytes=49 * 1024 * 1024
        ),
        name="fused",
    )(offsets, chirp_lengths, raw_first, raw_second, left, right, twist)
    return pl.pallas_call(
        store_kernel,
        out_shape=(
            jax.ShapeDtypeStruct((2, bins, lines), jnp.float32),
            jax.ShapeDtypeStruct((bins, lines), jnp.float32),
        ),
        in_specs=[vmem, vmem, vmem, vmem],
        out_specs=(hbm, hbm),
        scratch_shapes=[
            pltpu.VMEM((2, bins - early, lines), jnp.float32),
            pltpu.VMEM((bins - early, lines), jnp.float32),
            dma((2, 4)),
        ],
        compiler_params=pltpu.CompilerParams(vmem_limit_bytes=8 * 1024 * 1024),
        name="store",
    )(*held)


def solution(mesh):
    in_specs = (P("groups", "az", None), P("groups", "az", None), P("groups"), P("groups"))
    out_specs = (P("groups", "az", None), P(("groups", "az"), None))
    return jax.shard_map(
        on_device, mesh=mesh, in_specs=in_specs, out_specs=out_specs, check_vma=False
    )
```
